128 devices in a mesh: node: 8 (over y_hi, z), slab: 16 (over y_lo, x, core).
Axes of the slice: x: 4, y: 4 (y_hi: 2, y_lo: 2; y = y_hi * 2 + y_lo), z: 4, core: 2. Of those that a mesh axis runs over, the one named last changes fastest.
Arguments:
- initial: float32 [64, 256, 256], P('slab'), may hold values from -20 to 20
- sections: float32 [8, 64, 256, 256], P('node', 'slab'), may hold values from -21 to 21
Outputs:
- new_sections: float32 [8, 64, 256, 256], P('node', 'slab')
- residual_max: float32 [3], replicated
The draws below stay inside these ranges and needn't reach their ends.
All inputs are finite; a program needn't handle non-finite values.
Results may differ from the reference program's by a relative error of at most 0.0003.
Values sent between devices are 32-bit elements; how exact they have to be, the bound alone decides.
A program may use at most 64 MiB of HBM per device.

```python
import math
import jax
import jax.numpy as jnp
from jax import lax

M = 8
SWEEPS = 3
NY = 256
NZ = 256
NX = 64


def base_field(key):
    grid_shape = (NX, NY, NZ)
    position = jnp.arange(NX).astype(jnp.float32) / NX
    plane_scale = 10.0 ** (position - 0.5)
    factors = jax.random.uniform(jax.random.fold_in(key, 1), grid_shape, jnp.float32, 0.5, 1.5)
    values = jax.random.truncated_normal(jax.random.fold_in(key, 2), -4.0, 4.0, grid_shape, jnp.float32)
    return values * factors * plane_scale[:, None, None]


def draw_initial(key, part):
    return base_field(key)


def draw_sections(key, part):
    perturb = jax.random.truncated_normal(jax.random.fold_in(key, 3), -4.0, 4.0, (M, NX, NY, NZ), jnp.float32)
    return base_field(key)[None] + 0.2 * perturb


def setup_inputs(seed: int = 0) -> dict:
    seeds = jax.random.split(jax.random.key(seed), 3)
    initial = draw_initial(jax.random.fold_in(seeds[2], 71), 0)
    sections = draw_sections(jax.random.fold_in(seeds[2], 71), 0)
    return {"initial": initial, "sections": sections}


diffusion_step = 4.0


def radau_value(order, point):
    prev_value = 1.0
    prev_slope = 0.0
    this_value = point
    this_slope = 1.0
    for degree in range(1, order):
        next_value = ((2 * degree + 1) * point * this_value - degree * prev_value) / (degree + 1)
        next_slope = ((2 * degree + 1) * (this_value + point * this_slope) - degree * prev_slope) / (degree + 1)
        prev_value, prev_slope = this_value, this_slope
        this_value, this_slope = next_value, next_slope
    return this_value - prev_value, this_slope - prev_slope


def radau_tables(node_total):
    points = []
    for node_index in range(node_total):
        estimate = math.cos(2.0 * math.pi * node_index / (2 * node_total - 1))
        if node_index > 0:
            for repeat in range(60):
                poly_value, poly_slope = radau_value(node_total, estimate)
                estimate = estimate - poly_value / poly_slope
        points.append((estimate + 1.0) / 2.0)
    points = sorted(points)
    quadrature = []
    for row_index in range(node_total):
        entries = []
        for column_index in range(node_total):
            coeffs = [1.0]
            for other_index in range(node_total):
                if other_index != column_index:
                    divisor = points[column_index] - points[other_index]
                    shifted = [0.0] + coeffs
                    widened = coeffs + [0.0]
                    coeffs = [(shifted[place] - points[other_index] * widened[place]) / divisor for place in range(len(shifted))]
            integral = 0.0
            for place in range(len(coeffs)):
                integral = integral + coeffs[place] * points[row_index] ** (place + 1) / (place + 1)
            entries.append(integral)
        quadrature.append(entries)
    return points, quadrature


def laplacian(grid_values):
    beside = jnp.roll(grid_values, 1, 0) + jnp.roll(grid_values, -1, 0)
    beside = beside + jnp.roll(grid_values, 1, 1) + jnp.roll(grid_values, -1, 1)
    beside = beside + jnp.roll(grid_values, 1, 2) + jnp.roll(grid_values, -1, 2)
    return beside - 6.0 * grid_values


def eigen_line(length):
    indices = jnp.arange(length).astype(jnp.float32)
    return 2.0 * jnp.cos(indices * (2.0 * math.pi / length)) - 2.0


def reference(initial, sections):
    nodes_list, quad_list = radau_tables(M)
    nodes_at = jnp.asarray(nodes_list, jnp.float32)
    quadrature = jnp.asarray(quad_list, jnp.float32)
    spectrum = eigen_line(NX)[:, None, None] + eigen_line(NY)[None, :, None] + eigen_line(NZ)[None, None, :]
    current = sections
    maxima = []
    for sweep_index in range(SWEEPS):
        slopes = lax.map(laplacian, current)
        combined = jnp.einsum("mj,jxyz->mxyz", quadrature, slopes, precision=lax.Precision.HIGHEST)
        residual = initial[None] + diffusion_step * combined - current
        maxima.append(jnp.max(jnp.abs(residual)))
        diagonal = nodes_at / (sweep_index + 1.0)
        right_side = initial[None] + diffusion_step * (combined - diagonal[:, None, None, None] * slopes)

        def solve_one(pair):
            grid_values, weight = pair
            transformed = jnp.fft.fftn(grid_values)
            solved = jnp.fft.ifftn(transformed / (1.0 - diffusion_step * weight * spectrum))
            return jnp.real(solved).astype(jnp.float32)

        current = lax.map(solve_one, (right_side, diagonal))
    return current, jnp.stack(maxima)
```

```python
import functools
import math

import jax
import jax.numpy as jnp
import numpy as np
from jax import lax
from jax.experimental import pallas as pl
from jax.experimental.pallas import tpu as pltpu
from jax.sharding import Mesh
from jax.sharding import PartitionSpec as P

SWEEPS = 3
AXES = ("node_0", "node_1", "slab_0", "slab_1", "slab_2")
SLAB = ("slab_0", "slab_1", "slab_2")
NODE = ("node_0", "node_1")
MESH = pl.DeviceIdType.MESH
F32 = jnp.float32
BF16 = jnp.bfloat16
STEP = 4.0
NODES = 8
SLABS = 16
DEVS = NODES * SLABS
CELLS = 256
FIELDS = SWEEPS + 1


def radau_value(order, point):
    prev_value = 1.0
    prev_slope = 0.0
    this_value = point
    this_slope = 1.0
    for degree in range(1, order):
        next_value = ((2 * degree + 1) * point * this_value - degree * prev_value) / (degree + 1)
        next_slope = (
            (2 * degree + 1) * (this_value + point * this_slope) - degree * prev_slope
        ) / (degree + 1)
        prev_value, prev_slope = (this_value, this_slope)
        this_value, this_slope = (next_value, next_slope)
    return (this_value - prev_value, this_slope - prev_slope)


def radau_tables(node_total):
    points = []
    for node_index in range(node_total):
        estimate = math.cos(2.0 * math.pi * node_index / (2 * node_total - 1))
        if node_index > 0:
            for repeat in range(60):
                poly_value, poly_slope = radau_value(node_total, estimate)
                estimate = estimate - poly_value / poly_slope
        points.append((estimate + 1.0) / 2.0)
    points = sorted(points)
    quadrature = []
    for row_index in range(node_total):
        entries = []
        for column_index in range(node_total):
            coeffs = [1.0]
            for other_index in range(node_total):
                if other_index != column_index:
                    divisor = points[column_index] - points[other_index]
                    shifted = [0.0] + coeffs
                    widened = coeffs + [0.0]
                    coeffs = [
                        (shifted[place] - points[other_index] * widened[place]) / divisor
                        for place in range(len(shifted))
                    ]
            integral = 0.0
            for place in range(len(coeffs)):
                integral = integral + coeffs[place] * points[row_index] ** (place + 1) / (place + 1)
            entries.append(integral)
        quadrature.append(entries)
    return (points, quadrature)


def cas_table(length):
    indices = np.arange(length)
    phases = (indices[:, None] * indices[None, :] % length) * (2.0 * math.pi / length)
    return (np.cos(phases) + np.sin(phases)) / math.sqrt(length)


def eigen_line(length):
    return -4.0 * np.sin(np.arange(length) * (math.pi / length)) ** 2


def halves(table):
    high = table.astype(np.float32).astype(BF16)
    low = (table - high.astype(np.float64)).astype(np.float32).astype(BF16)
    return high, low


def tables():
    line = cas_table(CELLS)
    high, low = halves(line)
    right = np.concatenate([high, high, low], 0)
    left = np.concatenate([high, high, low], 1)
    cas_x = cas_table(64)
    cross = np.zeros((2, 64, SLABS, 2, 4))
    for row in range(2):
        cross[row, :, :, row, :] = cas_x.reshape(64, SLABS, 4)
    cross = cross.reshape(128, 128)
    high, low = halves(cross)
    forward = np.concatenate([high, high, low], 1)
    high, low = halves(cross.T)
    back = np.concatenate([high, high, low], 1)
    lam_x = np.broadcast_to((STEP * eigen_line(64))[:, None], (64, 128)).astype(np.float32)
    lam_z = np.broadcast_to((STEP * eigen_line(CELLS)).reshape(2, 1, 128), (2, 8, 128)).astype(np.float32)
    lam_y = (STEP * eigen_line(CELLS)).astype(np.float32)
    return right, left, forward, back, lam_x, lam_z, lam_y


def split(value, axis):
    high = value.astype(BF16)
    low = (value - high.astype(F32)).astype(BF16)
    return jnp.concatenate([high, low, high], axis)


def matmul(a, b):
    return jnp.dot(a, b, preferred_element_type=F32)


def kernel(
    points, quadrature,
    sec_hbm, ini_hbm, right_hbm, left_hbm, fwd_hbm, back_hbm, lam_x_hbm, lam_z_hbm, lam_y_ref,
    out_hbm, res_ref,
    sec, ini, right, left, fwd, back, lam_x, lam_z,
    rows, rows0, sent, sent0, got, got0, modes, modes0, spect, bsent, bgot, out, peak_sent, peak_got,
    in_sem, send_sem, send0_sem, got_sem, got0_sem, bsend_sem, bgot_sem, psend_sem, pgot_sem, out_sem,
):
    here = tuple(lax.axis_index(a) for a in AXES)
    my_node = here[0] * 4 + here[1]
    my_slab = (here[2] * 4 + here[3]) * 2 + here[4]
    me = my_node * SLABS + my_slab
    my_y = here[0] * 2 + here[2]

    loads = [
        pltpu.make_async_copy(src, dst, in_sem.at[i])
        for i, (src, dst) in enumerate([
            (left_hbm, left), (sec_hbm.at[0], sec), (right_hbm, right), (ini_hbm, ini), (fwd_hbm, fwd),
            (back_hbm, back), (lam_x_hbm, lam_x), (lam_z_hbm, lam_z),
        ])
    ]
    for load in loads:
        load.start()

    def target(k):
        y = lax.rem(my_y + k // 32, 4)
        return (
            y // 2,
            lax.rem(here[1] + lax.rem(k // 8, 4), 4),
            lax.rem(y, 2),
            lax.rem(here[3] + lax.rem(k // 2, 4), 4),
            lax.rem(here[4] + lax.rem(k, 2), 2),
        )

    def flat(t):
        return (((t[0] * 4 + t[1]) * 2 + t[2]) * 4 + t[3]) * 2 + t[4]

    barrier = pltpu.get_barrier_semaphore()

    def greet(k, carry):
        pl.semaphore_signal(barrier, inc=1, device_id=target(k), device_id_type=MESH)
        return carry

    lax.fori_loop(1, DEVS, greet, 0)

    def put(buf, x, count, value):
        for h in range(2):
            buf[h, pl.ds(x, count, stride=4), :] = value[:, 128 * h : 128 * h + 128]

    loads[0].wait()
    loads[1].wait()
    for x in range(4):
        put(rows, x, CELLS, matmul(left[...], split(sec[x], 0)))
    loads[2].wait()
    for b in range(4):
        part = jnp.concatenate([rows[h, pl.ds(CELLS * b, CELLS), :] for h in range(2)], 1)
        part = matmul(split(part, 1), right[...])
        for h in range(2):
            sent[h, pl.ds(32 * b, 32)] = part[:, 128 * h : 128 * h + 128].reshape(32, 8, 128)
    loads[3].wait()
    mine = left[pl.ds(pl.multiple_of(my_node * 32, 32), 32), :]
    for x in range(4):
        put(rows0, x, 32, matmul(mine, split(ini[x], 0)))
    part = jnp.concatenate([rows0[h] for h in range(2)], 1)
    part = matmul(split(part, 1), right[...])
    for h in range(2):
        sent0[h] = part[:, 128 * h : 128 * h + 128].reshape(16, 8, 128)

    pl.semaphore_wait(barrier, DEVS - 1)

    def spread(src, dst, s_sem, r_sem):
        def one(j, carry):
            t = target(lax.rem(j * 37, DEVS))
            pltpu.make_async_remote_copy(
                src.at[flat(t)], dst.at[me], s_sem, r_sem, device_id=t, device_id_type=MESH
            ).start()
            return carry

        lax.fori_loop(1, DEVS, one, 0)
        dst[me] = src[me]

    def all_but_one(buf, count, sem):
        view = buf.at[pl.ds(0, count - 1)]
        pltpu.make_async_copy(view, view, sem).wait()

    for h in range(2):
        def one(k, carry):
            yl = lax.rem(here[2] + k // 8, 2)
            x = lax.rem(here[3] + lax.rem(k // 2, 4), 4)
            c = lax.rem(here[4] + lax.rem(k, 2), 2)
            pltpu.make_async_remote_copy(
                sent0.at[h, (yl * 4 + x) * 2 + c], got0.at[h, my_slab], send0_sem.at[h], got0_sem.at[h],
                device_id=(here[0], here[1], yl, x, c), device_id_type=MESH,
            ).start()
            return carry

        lax.fori_loop(1, SLABS, one, 0)
        got0[h, my_slab] = sent0[h, my_slab]
        spread(sent.at[h], got.at[h], send_sem.at[h], got_sem.at[h])

    for load in loads[4:]:
        load.wait()

    def sweeps(h):
        all_but_one(got0.at[h], SLABS, got0_sem.at[h])
        all_but_one(got.at[h], DEVS, got_sem.at[h])
        modes0[...] = matmul(fwd[...], split(got0[h].reshape(128, 128), 0))
        for n in range(NODES):
            block = got[h, pl.ds(SLABS * n, SLABS)].reshape(128, 128)
            modes[:, 128 * n : 128 * n + 128] = matmul(fwd[...], split(block, 0))
        for row in range(2):
            lam_y = lam_y_ref[2 * me + row]

            def one(i, carry):
                r = pl.multiple_of(64 * row + 8 * i, 8)
                lam = lam_x[pl.ds(pl.multiple_of(8 * i, 8), 8), :] + lam_z[h] + lam_y
                start = modes0[pl.ds(r, 8), :]
                value = [modes[pl.ds(r, 8), 128 * m : 128 * m + 128] for m in range(NODES)]
                for k in range(SWEEPS):
                    slope = [lam * v for v in value]
                    after = []
                    for m in range(NODES):
                        total = start - value[m]
                        for j in range(NODES):
                            total = total + quadrature[m][j] * slope[j]
                        spect[k, pl.ds(r, 8), 128 * m : 128 * m + 128] = total
                        after.append(value[m] + total / (1.0 - (points[m] / (k + 1.0)) * lam))
                    value = after
                for m in range(NODES):
                    spect[SWEEPS, pl.ds(r, 8), 128 * m : 128 * m + 128] = value[m]
                return carry

            lax.fori_loop(0, 8, one, 0)

    def give(f, h):
        for n in range(NODES):
            block = matmul(back[...], split(spect[f, :, 128 * n : 128 * n + 128], 0))
            bsent[f, h, pl.ds(SLABS * n, SLABS)] = block.reshape(SLABS, 8, 128)
        spread(bsent.at[f, h], bgot.at[f, h], bsend_sem.at[f, h], bgot_sem.at[f, h])

    for h in range(2):
        sweeps(h)
        for f in range(FIELDS):
            give(f, h)

    def take(f):
        for h in range(2):
            all_but_one(bgot.at[f, h], DEVS, bgot_sem.at[f, h])
        for b in range(4):
            part = jnp.concatenate(
                [bgot[f, h, pl.ds(32 * b, 32)].reshape(CELLS, 128) for h in range(2)], 1
            )
            part = matmul(split(part, 1), right[...])
            for h in range(2):
                rows[h, pl.ds(CELLS * b, CELLS), :] = part[:, 128 * h : 128 * h + 128]
        for x in range(4):
            part = jnp.concatenate([rows[h, pl.ds(x, CELLS, stride=4), :] for h in range(2)], 1)
            yield x, matmul(left[...], split(part, 0))

    lane = lax.broadcasted_iota(jnp.int32, (1, 128), 1)
    peaks = jnp.zeros((1, 128), F32)
    for f in range(SWEEPS):
        top = None
        for x, field in take(f):
            field = jnp.max(jnp.abs(field).reshape(32, 8, CELLS), axis=0)
            top = field if top is None else jnp.maximum(top, field)
        peaks = jnp.where(lane == f, jnp.max(top), peaks)
    peak_sent[...] = peaks

    def tell(j, carry):
        pltpu.make_async_remote_copy(
            peak_sent, peak_got.at[me], psend_sem, pgot_sem,
            device_id=target(lax.rem(j * 37, DEVS)), device_id_type=MESH,
        ).start()
        return carry

    lax.fori_loop(1, DEVS, tell, 0)
    peak_got[me] = peaks
    for x, field in take(SWEEPS):
        out[x] = field
        pltpu.make_async_copy(out.at[x], out_hbm.at[0, x], out_sem.at[x]).start()

    all_but_one(peak_got, DEVS, pgot_sem)
    peaks = jnp.max(peak_got[...], axis=0)
    for f in range(SWEEPS):
        res_ref[f] = jnp.max(jnp.where(lane == f, peaks, 0.0))

    for h in range(2):
        all_but_one(sent0.at[h], SLABS, send0_sem.at[h])
        all_but_one(sent.at[h], DEVS, send_sem.at[h])
        for f in range(FIELDS):
            all_but_one(bsent.at[f, h], DEVS, bsend_sem.at[f, h])
    all_but_one(peak_got, DEVS, psend_sem)
    for x in range(4):
        pltpu.make_async_copy(out.at[x], out_hbm.at[0, x], out_sem.at[x]).wait()


def on_device(initial, sections):
    points, quadrature = radau_tables(NODES)
    any_space = pl.BlockSpec(memory_space=pl.ANY)
    smem = pl.BlockSpec(memory_space=pltpu.SMEM)
    dma = pltpu.SemaphoreType.DMA
    parts = [jnp.asarray(t) for t in tables()]
    vmem = pltpu.VMEM
    new, peak = pl.pallas_call(
        functools.partial(kernel, points, quadrature),
        out_shape=(
            jax.ShapeDtypeStruct(sections.shape, F32),
            jax.ShapeDtypeStruct((SWEEPS,), F32),
        ),
        in_specs=[any_space] * 8 + [smem],
        out_specs=(any_space, smem),
        scratch_shapes=[
            vmem((4, CELLS, CELLS), F32),
            vmem((4, CELLS, CELLS), F32),
            vmem((3 * CELLS, CELLS), BF16),
            vmem((CELLS, 3 * CELLS), BF16),
            vmem((128, 384), BF16),
            vmem((128, 384), BF16),
            vmem((64, 128), F32),
            vmem((2, 8, 128), F32),
            vmem((2, 4 * CELLS, 128), F32),
            vmem((2, 128, 128), F32),
            vmem((2, DEVS, 8, 128), F32),
            vmem((2, SLABS, 8, 128), F32),
            vmem((2, DEVS, 8, 128), F32),
            vmem((2, SLABS, 8, 128), F32),
            vmem((128, NODES * 128), F32),
            vmem((128, 128), F32),
            vmem((FIELDS, 128, NODES * 128), F32),
            vmem((FIELDS, 2, DEVS, 8, 128), F32),
            vmem((FIELDS, 2, DEVS, 8, 128), F32),
            vmem((4, CELLS, CELLS), F32),
            vmem((1, 128), F32),
            vmem((DEVS, 1, 128), F32),
            dma((8,)),
            dma((2,)),
            dma((2,)),
            dma((2,)),
            dma((2,)),
            dma((FIELDS, 2)),
            dma((FIELDS, 2)),
            dma,
            dma,
            dma((4,)),
        ],
        compiler_params=pltpu.CompilerParams(
            collective_id=0, has_side_effects=True, vmem_limit_bytes=48 << 20
        ),
        name="sdc",
    )(sections, initial, *parts)
    return new, peak


def solution(mesh):
    torus = Mesh(mesh.devices.reshape(2, 4, 2, 4, 2), AXES)
    return jax.shard_map(
        on_device,
        mesh=torus,
        in_specs=(P(SLAB, None, None), P(NODE, SLAB, None, None)),
        out_specs=(P(NODE, SLAB, None, None), P()),
        check_vma=False,
    )
```

```python
import functools
import math

import jax
import jax.numpy as jnp
import numpy as np
from jax import lax
from jax.experimental import pallas as pl
from jax.experimental.pallas import tpu as pltpu
from jax.sharding import Mesh
from jax.sharding import PartitionSpec as P

SWEEPS = 3
AXES = ("node_0", "node_1", "slab_0", "slab_1", "slab_2")
SLAB = ("slab_0", "slab_1", "slab_2")
NODE = ("node_0", "node_1")
MESH = pl.DeviceIdType.MESH
F32 = jnp.float32
BF16 = jnp.bfloat16
STEP = 4.0
NODES = 8
SLABS = 16
DEVS = NODES * SLABS
CELLS = 256
FIELDS = SWEEPS + 1


def radau_value(order, point):
    prev_value = 1.0
    prev_slope = 0.0
    this_value = point
    this_slope = 1.0
    for degree in range(1, order):
        next_value = ((2 * degree + 1) * point * this_value - degree * prev_value) / (degree + 1)
        next_slope = (
            (2 * degree + 1) * (this_value + point * this_slope) - degree * prev_slope
        ) / (degree + 1)
        prev_value, prev_slope = (this_value, this_slope)
        this_value, this_slope = (next_value, next_slope)
    return (this_value - prev_value, this_slope - prev_slope)


def radau_tables(node_total):
    points = []
    for node_index in range(node_total):
        estimate = math.cos(2.0 * math.pi * node_index / (2 * node_total - 1))
        if node_index > 0:
            for repeat in range(60):
                poly_value, poly_slope = radau_value(node_total, estimate)
                estimate = estimate - poly_value / poly_slope
        points.append((estimate + 1.0) / 2.0)
    points = sorted(points)
    quadrature = []
    for row_index in range(node_total):
        entries = []
        for column_index in range(node_total):
            coeffs = [1.0]
            for other_index in range(node_total):
                if other_index != column_index:
                    divisor = points[column_index] - points[other_index]
                    shifted = [0.0] + coeffs
                    widened = coeffs + [0.0]
                    coeffs = [
                        (shifted[place] - points[other_index] * widened[place]) / divisor
                        for place in range(len(shifted))
                    ]
            integral = 0.0
            for place in range(len(coeffs)):
                integral = integral + coeffs[place] * points[row_index] ** (place + 1) / (place + 1)
            entries.append(integral)
        quadrature.append(entries)
    return (points, quadrature)


def cas_table(length):
    indices = np.arange(length)
    phases = (indices[:, None] * indices[None, :] % length) * (2.0 * math.pi / length)
    return (np.cos(phases) + np.sin(phases)) / math.sqrt(length)


def eigen_line(length):
    return -4.0 * np.sin(np.arange(length) * (math.pi / length)) ** 2


def halves(table):
    high = table.astype(np.float32).astype(BF16)
    low = (table - high.astype(np.float64)).astype(np.float32).astype(BF16)
    return high, low


def tables():
    line = cas_table(CELLS)
    high, low = halves(line)
    right = np.concatenate([high, high, low], 0)
    left = np.concatenate([high, high, low], 1)
    cas_x = cas_table(64)
    cross = np.zeros((2, 64, SLABS, 2, 4))
    for row in range(2):
        cross[row, :, :, row, :] = cas_x.reshape(64, SLABS, 4)
    cross = cross.reshape(128, 128)
    high, low = halves(cross)
    forward = np.concatenate([high, high, low], 1)
    high, low = halves(cross.T)
    back = np.concatenate([high, high, low], 1)
    lam_x = np.broadcast_to((STEP * eigen_line(64))[:, None], (64, 128)).astype(np.float32)
    lam_z = np.broadcast_to((STEP * eigen_line(CELLS)).reshape(2, 1, 128), (2, 8, 128)).astype(np.float32)
    lam_y = np.broadcast_to((STEP * eigen_line(CELLS)).reshape(DEVS, 2, 1), (DEVS, 2, 128)).astype(np.float32)
    return right, left, forward, back, lam_x, lam_z, lam_y


def split(value, axis):
    high = value.astype(BF16)
    low = (value - high.astype(F32)).astype(BF16)
    return jnp.concatenate([high, low, high], axis)


def matmul(a, b):
    return jnp.dot(a, b, preferred_element_type=F32)


def kernel(
    points, quadrature,
    sec_hbm, ini_hbm, right_hbm, left_hbm, fwd_hbm, back_hbm, lam_x_hbm, lam_z_hbm, lam_y_hbm,
    out_hbm, res_ref,
    sec, ini, right, left, fwd, back, lam_x, lam_z, lam_y,
    rows, rows0, sent, sent0, got, got0, modes, modes0, spect, bsent, bgot, out, peak_sent, peak_got,
    in_sem, send_sem, send0_sem, got_sem, got0_sem, bsend_sem, bgot_sem, psend_sem, pgot_sem, out_sem,
):
    here = tuple(lax.axis_index(a) for a in AXES)
    my_node = here[0] * 4 + here[1]
    my_slab = (here[2] * 4 + here[3]) * 2 + here[4]
    me = my_node * SLABS + my_slab
    my_y = here[0] * 2 + here[2]

    loads = [
        pltpu.make_async_copy(src, dst, in_sem.at[i])
        for i, (src, dst) in enumerate([
            (left_hbm, left), (sec_hbm.at[0], sec), (right_hbm, right), (ini_hbm, ini), (fwd_hbm, fwd),
            (back_hbm, back), (lam_x_hbm, lam_x), (lam_z_hbm, lam_z), (lam_y_hbm.at[me], lam_y),
        ])
    ]
    for load in loads:
        load.start()

    def flat(t):
        return (((t[0] * 4 + t[1]) * 2 + t[2]) * 4 + t[3]) * 2 + t[4]

    cores = (here[4], 1 - here[4])
    planes = [lax.rem(my_y + k, 4) for k in range(4)]
    planes = [(y // 2, lax.rem(y, 2)) for y in planes]
    depths = [lax.rem(here[1] + k, 4) for k in range(4)]

    def others(visit, low=0, high=4):
        def step(i, first):
            along = [lax.rem(here[3] + i + k, 4) for k in range(4)]
            for k in range(first, 32):
                y_high, y_low = planes[5 * k % 16 // 4]
                visit((y_high, depths[5 * k % 4], y_low, along[k % 4], cores[k // 16]))

        def body(i, carry):
            step(i, 0)
            return carry

        if low == 0:
            step(0, 1)
        lax.fori_loop(max(low, 1), high, body, 0)

    barrier = pltpu.get_barrier_semaphore()

    others(lambda t: pl.semaphore_signal(barrier, inc=1, device_id=t, device_id_type=MESH))

    def put(buf, x, count, value):
        for h in range(2):
            buf[h, pl.ds(x, count, stride=4), :] = value[:, 128 * h : 128 * h + 128]

    loads[0].wait()
    loads[1].wait()
    for x in range(4):
        put(rows, x, CELLS, matmul(left[...], split(sec[x], 0)))
    loads[2].wait()
    for b in range(4):
        part = jnp.concatenate([rows[h, pl.ds(CELLS * b, CELLS), :] for h in range(2)], 1)
        part = matmul(split(part, 1), right[...])
        for h in range(2):
            sent[h, pl.ds(32 * b, 32)] = part[:, 128 * h : 128 * h + 128].reshape(32, 8, 128)
    pl.semaphore_wait(barrier, DEVS - 1)

    def spread(src, dst, s_sem, r_sem, low=0, high=4):
        others(
            lambda t: pltpu.make_async_remote_copy(
                src.at[flat(t)], dst.at[me], s_sem, r_sem, device_id=t, device_id_type=MESH
            ).start(),
            low, high,
        )
        if low == 0:
            dst[me] = src[me]

    def all_but_one(buf, count, sem):
        view = buf.at[pl.ds(0, count - 1)]
        pltpu.make_async_copy(view, view, sem).wait()

    spread(sent.at[0], got.at[0], send_sem.at[0], got_sem.at[0])
    loads[3].wait()
    mine = left[pl.ds(pl.multiple_of(my_node * 32, 32), 32), :]
    for x in range(4):
        put(rows0, x, 32, matmul(mine, split(ini[x], 0)))
    part = jnp.concatenate([rows0[h] for h in range(2)], 1)
    part = matmul(split(part, 1), right[...])
    for h in range(2):
        sent0[h] = part[:, 128 * h : 128 * h + 128].reshape(16, 8, 128)

    for h in range(2):
        for k in range(1, SLABS):
            x = lax.rem(here[3] + k, 4)
            t = (here[0], here[1], here[2] if k < 8 else 1 - here[2], x, cores[k // 4 % 2])
            pltpu.make_async_remote_copy(
                sent0.at[h, (t[2] * 4 + t[3]) * 2 + t[4]], got0.at[h, my_slab], send0_sem.at[h], got0_sem.at[h],
                device_id=t, device_id_type=MESH,
            ).start()
        got0[h, my_slab] = sent0[h, my_slab]
    spread(sent.at[1], got.at[1], send_sem.at[1], got_sem.at[1])

    for load in loads[4:]:
        load.wait()

    def sweeps(h):
        all_but_one(got0.at[h], SLABS, got0_sem.at[h])
        all_but_one(got.at[h], DEVS, got_sem.at[h])
        modes0[...] = matmul(fwd[...], split(got0[h].reshape(128, 128), 0))
        for n in range(NODES):
            block = got[h, pl.ds(SLABS * n, SLABS)].reshape(128, 128)
            modes[:, 128 * n : 128 * n + 128] = matmul(fwd[...], split(block, 0))
        for row in range(2):
            lam_0 = lam_z[h] + lam_y[row : row + 1, :]

            def one(i, carry):
                r = pl.multiple_of(64 * row + 8 * i, 8)
                lam = lam_x[pl.ds(pl.multiple_of(8 * i, 8), 8), :] + lam_0
                start = modes0[pl.ds(r, 8), :]
                value = [modes[pl.ds(r, 8), 128 * m : 128 * m + 128] for m in range(NODES)]
                for k in range(SWEEPS):
                    slope = [lam * v for v in value]
                    after = []
                    for m in range(NODES):
                        total = start - value[m]
                        for j in range(NODES):
                            total = total + quadrature[m][j] * slope[j]
                        spect[k, pl.ds(r, 8), 128 * m : 128 * m + 128] = total
                        after.append(value[m] + total / (1.0 - (points[m] / (k + 1.0)) * lam))
                    value = after
                for m in range(NODES):
                    spect[SWEEPS, pl.ds(r, 8), 128 * m : 128 * m + 128] = value[m]
                return carry

            lax.fori_loop(0, 8, one, 0)

    def make(f, h):
        for n in range(NODES):
            block = matmul(back[...], split(spect[f, :, 128 * n : 128 * n + 128], 0))
            bsent[f, h, pl.ds(SLABS * n, SLABS)] = block.reshape(SLABS, 8, 128)

    def give(f, h, low=0, high=4):
        spread(bsent.at[f, h], bgot.at[f, h], bsend_sem.at[f, h], bgot_sem.at[f, h], low, high)

    sweeps(0)
    for f in range(2):
        make(f, 0)
        give(f, 0)
    for f in range(2, FIELDS):
        make(f, 0)
    sweeps(1)
    for f in range(FIELDS):
        make(f, 1)
        if f >= 2:
            give(f, 0)
        give(f, 1, 0, 4 if f < SWEEPS else 2)

    def take(f):
        for h in range(2):
            all_but_one(bgot.at[f, h], DEVS, bgot_sem.at[f, h])
        for b in range(4):
            part = jnp.concatenate(
                [bgot[f, h, pl.ds(32 * b, 32)].reshape(CELLS, 128) for h in range(2)], 1
            )
            part = matmul(split(part, 1), right[...])
            for h in range(2):
                rows[h, pl.ds(CELLS * b, CELLS), :] = part[:, 128 * h : 128 * h + 128]
        for x in range(4):
            part = jnp.concatenate([rows[h, pl.ds(x, CELLS, stride=4), :] for h in range(2)], 1)
            yield x, matmul(left[...], split(part, 0))

    lane = lax.broadcasted_iota(jnp.int32, (1, 128), 1)
    peaks = jnp.zeros((1, 128), F32)
    for f in range(SWEEPS):
        top = None
        for x, field in take(f):
            field = jnp.max(jnp.abs(field).reshape(32, 8, CELLS), axis=0)
            top = field if top is None else jnp.maximum(top, field)
        peaks = jnp.where(lane == f, jnp.max(top), peaks)
    peak_sent[...] = peaks

    others(
        lambda t: pltpu.make_async_remote_copy(
            peak_sent, peak_got.at[me], psend_sem, pgot_sem, device_id=t, device_id_type=MESH
        ).start()
    )
    peak_got[me] = peaks
    give(SWEEPS, 1, 2, 4)
    for x, field in take(SWEEPS):
        out[x] = field
        pltpu.make_async_copy(out.at[x], out_hbm.at[0, x], out_sem.at[x]).start()

    all_but_one(peak_got, DEVS, pgot_sem)
    peaks = jnp.max(peak_got[...], axis=0)
    for f in range(SWEEPS):
        res_ref[f] = jnp.max(jnp.where(lane == f, peaks, 0.0))

    for h in range(2):
        all_but_one(sent0.at[h], SLABS, send0_sem.at[h])
        all_but_one(sent.at[h], DEVS, send_sem.at[h])
        for f in range(FIELDS):
            all_but_one(bsent.at[f, h], DEVS, bsend_sem.at[f, h])
    all_but_one(peak_got, DEVS, psend_sem)
    for x in range(4):
        pltpu.make_async_copy(out.at[x], out_hbm.at[0, x], out_sem.at[x]).wait()


def on_device(initial, sections):
    points, quadrature = radau_tables(NODES)
    any_space = pl.BlockSpec(memory_space=pl.ANY)
    smem = pl.BlockSpec(memory_space=pltpu.SMEM)
    dma = pltpu.SemaphoreType.DMA
    parts = [jnp.asarray(t) for t in tables()]
    vmem = pltpu.VMEM
    new, peak = pl.pallas_call(
        functools.partial(kernel, points, quadrature),
        out_shape=(
            jax.ShapeDtypeStruct(sections.shape, F32),
            jax.ShapeDtypeStruct((SWEEPS,), F32),
        ),
        in_specs=[any_space] * 9,
        out_specs=(any_space, smem),
        scratch_shapes=[
            vmem((4, CELLS, CELLS), F32),
            vmem((4, CELLS, CELLS), F32),
            vmem((3 * CELLS, CELLS), BF16),
            vmem((CELLS, 3 * CELLS), BF16),
            vmem((128, 384), BF16),
            vmem((128, 384), BF16),
            vmem((64, 128), F32),
            vmem((2, 8, 128), F32),
            vmem((2, 128), F32),
            vmem((2, 4 * CELLS, 128), F32),
            vmem((2, 128, 128), F32),
            vmem((2, DEVS, 8, 128), F32),
            vmem((2, SLABS, 8, 128), F32),
            vmem((2, DEVS, 8, 128), F32),
            vmem((2, SLABS, 8, 128), F32),
            vmem((128, NODES * 128), F32),
            vmem((128, 128), F32),
            vmem((FIELDS, 128, NODES * 128), F32),
            vmem((FIELDS, 2, DEVS, 8, 128), F32),
            vmem((FIELDS, 2, DEVS, 8, 128), F32),
            vmem((4, CELLS, CELLS), F32),
            vmem((1, 128), F32),
            vmem((DEVS, 1, 128), F32),
            dma((9,)),
            dma((2,)),
            dma((2,)),
            dma((2,)),
            dma((2,)),
            dma((FIELDS, 2)),
            dma((FIELDS, 2)),
            dma,
            dma,
            dma((4,)),
        ],
        compiler_params=pltpu.CompilerParams(
            collective_id=0, has_side_effects=True, vmem_limit_bytes=67043328
        ),
        name="sdc",
    )(sections, initial, *parts)
    return new, peak


def solution(mesh):
    torus = Mesh(mesh.devices.reshape(2, 4, 2, 4, 2), AXES)
    return jax.shard_map(
        on_device,
        mesh=torus,
        in_specs=(P(SLAB, None, None), P(NODE, SLAB, None, None)),
        out_specs=(P(NODE, SLAB, None, None), P()),
        check_vma=False,
    )
```

```python
import functools
import math

import jax
import jax.numpy as jnp
import numpy as np
from jax import lax
from jax.experimental import pallas as pl
from jax.experimental.pallas import tpu as pltpu
from jax.sharding import Mesh
from jax.sharding import PartitionSpec as P

SWEEPS = 3
AXES = ("node_0", "node_1", "slab_0", "slab_1", "slab_2")
SLAB = ("slab_0", "slab_1", "slab_2")
NODE = ("node_0", "node_1")
MESH = pl.DeviceIdType.MESH
F32 = jnp.float32
BF16 = jnp.bfloat16
STEP = 4.0
NODES = 8
SLABS = 16
DEVS = NODES * SLABS
CELLS = 256
FIELDS = SWEEPS + 1
HOPS = (0, 1, 2, 1)
FAR_FIRST = sorted(
    ((k // 4 % 4, k % 4, (k + k // 16) % 4, k // 64) for k in (37 * j % DEVS for j in range(DEVS))),
    key=lambda offset: -sum(HOPS[step] for step in offset[:3]),
)
FAR_FIRST.remove((0, 0, 0, 0))


def radau_value(order, point):
    prev_value = 1.0
    prev_slope = 0.0
    this_value = point
    this_slope = 1.0
    for degree in range(1, order):
        next_value = ((2 * degree + 1) * point * this_value - degree * prev_value) / (degree + 1)
        next_slope = (
            (2 * degree + 1) * (this_value + point * this_slope) - degree * prev_slope
        ) / (degree + 1)
        prev_value, prev_slope = (this_value, this_slope)
        this_value, this_slope = (next_value, next_slope)
    return (this_value - prev_value, this_slope - prev_slope)


def radau_tables(node_total):
    points = []
    for node_index in range(node_total):
        estimate = math.cos(2.0 * math.pi * node_index / (2 * node_total - 1))
        if node_index > 0:
            for repeat in range(60):
                poly_value, poly_slope = radau_value(node_total, estimate)
                estimate = estimate - poly_value / poly_slope
        points.append((estimate + 1.0) / 2.0)
    points = sorted(points)
    quadrature = []
    for row_index in range(node_total):
        entries = []
        for column_index in range(node_total):
            coeffs = [1.0]
            for other_index in range(node_total):
                if other_index != column_index:
                    divisor = points[column_index] - points[other_index]
                    shifted = [0.0] + coeffs
                    widened = coeffs + [0.0]
                    coeffs = [
                        (shifted[place] - points[other_index] * widened[place]) / divisor
                        for place in range(len(shifted))
                    ]
            integral = 0.0
            for place in range(len(coeffs)):
                integral = integral + coeffs[place] * points[row_index] ** (place + 1) / (place + 1)
            entries.append(integral)
        quadrature.append(entries)
    return (points, quadrature)


def cas_table(length):
    indices = np.arange(length)
    phases = (indices[:, None] * indices[None, :] % length) * (2.0 * math.pi / length)
    return (np.cos(phases) + np.sin(phases)) / math.sqrt(length)


def eigen_line(length):
    return -4.0 * np.sin(np.arange(length) * (math.pi / length)) ** 2


def halves(table):
    high = table.astype(np.float32).astype(BF16)
    low = (table - high.astype(np.float64)).astype(np.float32).astype(BF16)
    return high, low


def tables():
    line = cas_table(CELLS)
    high, low = halves(line)
    right = np.concatenate([part for h in (slice(0, 128), slice(128, 256)) for part in (high[h], high[h], low[h])], 0)
    left = np.concatenate([high, high, low], 1)
    cas_x = cas_table(64)
    cross = np.zeros((2, 64, SLABS, 2, 4))
    for row in range(2):
        cross[row, :, :, row, :] = cas_x.reshape(64, SLABS, 4)
    cross = cross.reshape(128, 128)
    high, low = halves(cross)
    forward = np.concatenate([high, high, low], 1)
    high, low = halves(cross.T)
    back = np.concatenate([high, high, low], 1)
    lam_x = np.broadcast_to((STEP * eigen_line(64))[:, None], (64, 128)).astype(np.float32)
    lam_z = np.broadcast_to((STEP * eigen_line(CELLS)).reshape(2, 1, 128), (2, 8, 128)).astype(np.float32)
    lam_y = np.broadcast_to((STEP * eigen_line(CELLS)).reshape(DEVS, 2, 1), (DEVS, 2, 128)).astype(np.float32)
    return right, left, forward, back, lam_x, lam_z, lam_y


def split(value, axis):
    high = value.astype(BF16)
    low = (value - high.astype(F32)).astype(BF16)
    return jnp.concatenate([high, low, high], axis)


def split_halves(first, second):
    return jnp.concatenate([split(first, 1), split(second, 1)], 1)


def matmul(a, b):
    return jnp.dot(a, b, preferred_element_type=F32)


def kernel(
    points, quadrature,
    sec_hbm, ini_hbm, right_hbm, left_hbm, fwd_hbm, back_hbm, lam_x_hbm, lam_z_hbm, lam_y_hbm,
    base, last, peak, right_b,
    sec, ini, right, left, fwd, back, lam_x, lam_z, lam_y,
    rows, rows0, sent, sent0, got, got0, modes, modes0, spect, bsent, bgot, peak_sent, peak_got,
    in_sem, send_sem, send0_sem, got_sem, got0_sem, bsend_sem, bgot_sem, psend_sem, pgot_sem,
):
    here = tuple(lax.axis_index(a) for a in AXES)
    my_node = here[0] * 4 + here[1]
    my_slab = (here[2] * 4 + here[3]) * 2 + here[4]
    me = my_node * SLABS + my_slab
    my_y = here[0] * 2 + here[2]

    loads = [
        pltpu.make_async_copy(src, dst, in_sem.at[i])
        for i, (src, dst) in enumerate([
            (left_hbm, left), (sec_hbm.at[0], sec), (right_hbm, right), (ini_hbm, ini), (fwd_hbm, fwd),
            (back_hbm, back), (lam_x_hbm, lam_x), (lam_z_hbm, lam_z), (lam_y_hbm.at[me], lam_y),
            (right_hbm.at[pl.ds(384, 384)], right_b),
        ])
    ]
    for load in loads:
        load.start()

    def flat(t):
        return (((t[0] * 4 + t[1]) * 2 + t[2]) * 4 + t[3]) * 2 + t[4]

    cores = (here[4], 1 - here[4])
    planes = [lax.rem(my_y + k, 4) for k in range(4)]
    planes = [(y // 2, lax.rem(y, 2)) for y in planes]
    across = [lax.rem(here[3] + k, 4) for k in range(4)]
    depths = [lax.rem(here[1] + k, 4) for k in range(4)]

    def others(visit, low=0, high=4):
        def step(i, first):
            along = [lax.rem(here[3] + i + k, 4) for k in range(4)]
            for k in range(first, 32):
                y_high, y_low = planes[5 * k % 16 // 4]
                visit((y_high, depths[5 * k % 4], y_low, along[k % 4], cores[k // 16]))

        def body(i, carry):
            step(i, 0)
            return carry

        if low == 0:
            step(0, 1)
        lax.fori_loop(max(low, 1), high, body, 0)

    def far_first(visit, low=0, high=DEVS - 1):
        for y, z, x, core in FAR_FIRST[low:high]:
            visit((planes[y][0], depths[z], planes[y][1], across[x], cores[core]))

    barrier = pltpu.get_barrier_semaphore()

    far_first(lambda t: pl.semaphore_signal(barrier, inc=1, device_id=t, device_id_type=MESH))

    def put(buf, x, count, value):
        for h in range(2):
            buf[h, pl.ds(x, count, stride=4), :] = value[:, 128 * h : 128 * h + 128]

    loads[0].wait()
    loads[1].wait()
    for x in range(4):
        put(rows, x, CELLS, matmul(left[...], split(sec[x], 0)))
    loads[2].wait()
    for b in range(4):
        part = split_halves(*(rows[h, pl.ds(CELLS * b, CELLS), :] for h in range(2)))
        part = matmul(part, right[...])
        for h in range(2):
            sent[h, pl.ds(32 * b, 32)] = part[:, 128 * h : 128 * h + 128].reshape(32, 8, 128)
    pl.semaphore_wait(barrier, DEVS - 1)

    def spread(src, dst, s_sem, r_sem, order=others, low=None, high=None):
        order(
            lambda t: pltpu.make_async_remote_copy(
                src.at[flat(t)], dst.at[me], s_sem, r_sem, device_id=t, device_id_type=MESH
            ).start(),
            *(() if low is None else (low, high)),
        )
        if not low:
            dst[me] = src[me]

    def all_but_one(buf, count, sem):
        view = buf.at[pl.ds(0, count - 1)]
        pltpu.make_async_copy(view, view, sem).wait()

    spread(sent.at[0], got.at[0], send_sem.at[0], got_sem.at[0])
    loads[3].wait()
    mine = left[pl.ds(pl.multiple_of(my_node * 32, 32), 32), :]
    for x in range(4):
        put(rows0, x, 32, matmul(mine, split(ini[x], 0)))
    part = matmul(split_halves(rows0[0], rows0[1]), right[...])
    for h in range(2):
        sent0[h] = part[:, 128 * h : 128 * h + 128].reshape(16, 8, 128)

    for h in range(2):
        for k in range(1, SLABS):
            x = lax.rem(here[3] + k, 4)
            t = (here[0], here[1], here[2] if k < 8 else 1 - here[2], x, cores[k // 4 % 2])
            pltpu.make_async_remote_copy(
                sent0.at[h, (t[2] * 4 + t[3]) * 2 + t[4]], got0.at[h, my_slab], send0_sem.at[h], got0_sem.at[h],
                device_id=t, device_id_type=MESH,
            ).start()
        got0[h, my_slab] = sent0[h, my_slab]
    spread(sent.at[1], got.at[1], send_sem.at[1], got_sem.at[1])

    for load in loads[4:9]:
        load.wait()

    def enter(h):
        all_but_one(got0.at[h], SLABS, got0_sem.at[h])
        all_but_one(got.at[h], DEVS, got_sem.at[h])
        modes0[...] = matmul(fwd[...], split(got0[h].reshape(128, 128), 0))
        for n in range(0, NODES, 2):
            pair = [got[h, pl.ds(SLABS * (n + k), SLABS)].reshape(128, 128) for k in range(2)]
            modes[:, 128 * n : 128 * n + 256] = matmul(fwd[...], split(jnp.concatenate(pair, 1), 0))

    def sweep(k, h):
        lam_0 = [lam_z[h] + lam_y[row : row + 1, :] for row in range(2)]

        def one(i, carry):
            lam_1 = lam_x[pl.ds(pl.multiple_of(8 * i, 8), 8), :]
            for row in range(2):
                r = pl.multiple_of(64 * row + 8 * i, 8)
                lam = lam_1 + lam_0[row]
                start = modes0[pl.ds(r, 8), :]
                value = [modes[pl.ds(r, 8), 128 * m : 128 * m + 128] for m in range(NODES)]
                slope = [lam * v for v in value]
                for m in range(NODES):
                    total = start - value[m]
                    for j in range(NODES):
                        total = total + quadrature[m][j] * slope[j]
                    spect[pl.ds(r, 8), 128 * m : 128 * m + 128] = total
                    modes[pl.ds(r, 8), 128 * m : 128 * m + 128] = value[m] + total / (
                        1.0 - (points[m] / (k + 1.0)) * lam
                    )
            return carry

        lax.fori_loop(0, 8, one, 0)

    def make(f, h):
        source = spect if f < SWEEPS else modes
        for n in range(0, NODES, 2):
            pair = matmul(back[...], split(source[:, 128 * n : 128 * n + 256], 0))
            for k in range(2):
                block = pair[:, 128 * k : 128 * k + 128].reshape(SLABS, 8, 128)
                bsent[f, h, pl.ds(SLABS * (n + k), SLABS)] = block

    def give(f, h, *how):
        spread(bsent.at[f, h], bgot.at[f, h], bsend_sem.at[f, h], bgot_sem.at[f, h], *how)

    enter(0)
    for f in range(FIELDS):
        if f < SWEEPS:
            sweep(f, 0)
        make(f, 0)
        if f < 2:
            give(f, 0)
    enter(1)
    for f in range(FIELDS):
        if f < SWEEPS:
            sweep(f, 1)
        make(f, 1)
        if f >= 2:
            give(f, 0)
        give(f, 1, *(() if f < SWEEPS else (far_first, 0, 48)))

    def ready(f, h):
        all_but_one(bgot.at[f, h], DEVS, bgot_sem.at[f, h])

    def plane(f, h, x):
        return bgot.at[f, h].reshape(4 * CELLS, 128)[pl.ds(x, CELLS, stride=4), :]

    def pairs(h):
        for x in range(0, 4, 2):
            part = jnp.concatenate([plane(SWEEPS, h, x + k) for k in range(2)], 1)
            part = matmul(left[...], split(part, 0))
            yield x, part[:, :128]
            yield x + 1, part[:, 128:]

    lane = lax.broadcasted_iota(jnp.int32, (1, 128), 1)
    peaks = jnp.zeros((1, 128), F32)
    for f in range(SWEEPS):
        ready(f, 0)
        ready(f, 1)
        top = None
        for x in range(4):
            part = jnp.concatenate([plane(f, h, x) for h in range(2)], 1)
            part = matmul(left[...], split(part, 0))
            part = matmul(split_halves(part[:, :128], part[:, 128:]), right[...])
            part = jnp.max(jnp.abs(part).reshape(32, 8, CELLS), axis=0)
            top = part if top is None else jnp.maximum(top, part)
        peaks = jnp.where(lane == f, jnp.max(top), peaks)
    peak_sent[...] = peaks

    far_first(
        lambda t: pltpu.make_async_remote_copy(
            peak_sent, peak_got.at[me], psend_sem, pgot_sem, device_id=t, device_id_type=MESH
        ).start()
    )
    peak_got[me] = peaks
    give(SWEEPS, 1, far_first, 48, DEVS - 1)
    ready(SWEEPS, 0)
    for x, part in pairs(0):
        base[x] = matmul(split(part, 1), right[pl.ds(0, 384), :])
    all_but_one(peak_got, DEVS, pgot_sem)
    peak[...] = jnp.max(peak_got[...], axis=0)
    for h in range(2):
        all_but_one(sent0.at[h], SLABS, send0_sem.at[h])
        all_but_one(sent.at[h], DEVS, send_sem.at[h])
        for f in range(FIELDS):
            all_but_one(bsent.at[f, h], DEVS, bsend_sem.at[f, h])
    all_but_one(peak_got, DEVS, psend_sem)
    loads[9].wait()
    ready(SWEEPS, 1)
    for x, part in pairs(1):
        last[x] = part


def finish(base, last, peak, right_b, out_hbm, res_hbm, out, res, out_sem):
    copies = [pltpu.make_async_copy(out.at[x], out_hbm.at[0, x], out_sem.at[x]) for x in range(4)]
    for x in range(4):
        out[x] = base[x] + matmul(split(last[x], 1), right_b[...])
        copies[x].start()
        if x == 0:
            lane = lax.broadcasted_iota(jnp.int32, (1, 128), 1)
            for f in range(SWEEPS):
                res[f] = jnp.max(jnp.where(lane == f, peak[...], 0.0))
            copies.append(pltpu.make_async_copy(res, res_hbm, out_sem.at[4]))
            copies[4].start()
    for copy in copies:
        copy.wait()


def on_device(initial, sections):
    points, quadrature = radau_tables(NODES)
    any_space = pl.BlockSpec(memory_space=pl.ANY)
    dma = pltpu.SemaphoreType.DMA
    parts = [jnp.asarray(t) for t in tables()]
    vmem = pltpu.VMEM
    whole = pl.BlockSpec(memory_space=pltpu.VMEM)
    pinned = pl.BlockSpec(memory_space=pltpu.HBM)
    found = pl.pallas_call(
        functools.partial(kernel, points, quadrature),
        out_shape=(
            jax.ShapeDtypeStruct((4, CELLS, CELLS), F32),
            jax.ShapeDtypeStruct((4, CELLS, 128), F32),
            jax.ShapeDtypeStruct((1, 128), F32),
            jax.ShapeDtypeStruct((384, CELLS), BF16),
        ),
        in_specs=[pinned] * 9,
        out_specs=(whole,) * 4,
        scratch_shapes=[
            vmem((4, CELLS, CELLS), F32),
            vmem((4, CELLS, CELLS), F32),
            vmem((3 * CELLS, CELLS), BF16),
            vmem((CELLS, 3 * CELLS), BF16),
            vmem((128, 384), BF16),
            vmem((128, 384), BF16),
            vmem((64, 128), F32),
            vmem((2, 8, 128), F32),
            vmem((2, 128), F32),
            vmem((2, 4 * CELLS, 128), F32),
            vmem((2, 128, 128), F32),
            vmem((2, DEVS, 8, 128), F32),
            vmem((2, SLABS, 8, 128), F32),
            vmem((2, DEVS, 8, 128), F32),
            vmem((2, SLABS, 8, 128), F32),
            vmem((128, NODES * 128), F32),
            vmem((128, 128), F32),
            vmem((128, NODES * 128), F32),
            vmem((FIELDS, 2, DEVS, 8, 128), F32),
            vmem((FIELDS, 2, DEVS, 8, 128), F32),
            vmem((1, 128), F32),
            vmem((DEVS, 1, 128), F32),
            dma((10,)),
            dma((2,)),
            dma((2,)),
            dma((2,)),
            dma((2,)),
            dma((FIELDS, 2)),
            dma((FIELDS, 2)),
            dma,
            dma,
        ],
        compiler_params=pltpu.CompilerParams(
            collective_id=0, has_side_effects=True, vmem_limit_bytes=30 << 20
        ),
        name="sdc",
    )(*(pltpu.with_memory_space_constraint(value, pltpu.HBM) for value in (sections, initial, *parts)))
    return pl.pallas_call(
        finish,
        out_shape=(
            jax.ShapeDtypeStruct(sections.shape, F32),
            jax.ShapeDtypeStruct((SWEEPS,), F32),
        ),
        in_specs=[whole] * 4,
        out_specs=(any_space, any_space),
        scratch_shapes=[vmem((4, CELLS, CELLS), F32), pltpu.SMEM((SWEEPS,), F32), dma((5,))],
        compiler_params=pltpu.CompilerParams(vmem_limit_bytes=16 << 20),
        name="finish",
    )(*found)


def solution(mesh):
    torus = Mesh(mesh.devices.reshape(2, 4, 2, 4, 2), AXES)
    return jax.shard_map(
        on_device,
        mesh=torus,
        in_specs=(P(SLAB, None, None), P(NODE, SLAB, None, None)),
        out_specs=(P(NODE, SLAB, None, None), P()),
        check_vma=False,
    )
```

```python
import functools
import math

import jax
import jax.numpy as jnp
import numpy as np
from jax import lax
from jax.experimental import pallas as pl
from jax.experimental.pallas import tpu as pltpu
from jax.sharding import Mesh
from jax.sharding import PartitionSpec as P

SWEEPS = 3
AXES = ("node_0", "node_1", "slab_0", "slab_1", "slab_2")
SLAB = ("slab_0", "slab_1", "slab_2")
NODE = ("node_0", "node_1")
MESH = pl.DeviceIdType.MESH
F32 = jnp.float32
BF16 = jnp.bfloat16
STEP = 4.0
NODES = 8
SLABS = 16
DEVS = NODES * SLABS
CELLS = 256
FIELDS = SWEEPS + 1
HOPS = (0, 1, 2, 1)
FAR_FIRST = sorted(
    ((k // 4 % 4, k % 4, (k + k // 16) % 4, k // 64) for k in (37 * j % DEVS for j in range(DEVS))),
    key=lambda offset: -sum(HOPS[step] for step in offset[:3]),
)
FAR_FIRST.remove((0, 0, 0, 0))


def radau_value(order, point):
    prev_value = 1.0
    prev_slope = 0.0
    this_value = point
    this_slope = 1.0
    for degree in range(1, order):
        next_value = ((2 * degree + 1) * point * this_value - degree * prev_value) / (degree + 1)
        next_slope = (
            (2 * degree + 1) * (this_value + point * this_slope) - degree * prev_slope
        ) / (degree + 1)
        prev_value, prev_slope = (this_value, this_slope)
        this_value, this_slope = (next_value, next_slope)
    return (this_value - prev_value, this_slope - prev_slope)


def radau_tables(node_total):
    points = []
    for node_index in range(node_total):
        estimate = math.cos(2.0 * math.pi * node_index / (2 * node_total - 1))
        if node_index > 0:
            for repeat in range(60):
                poly_value, poly_slope = radau_value(node_total, estimate)
                estimate = estimate - poly_value / poly_slope
        points.append((estimate + 1.0) / 2.0)
    points = sorted(points)
    quadrature = []
    for row_index in range(node_total):
        entries = []
        for column_index in range(node_total):
            coeffs = [1.0]
            for other_index in range(node_total):
                if other_index != column_index:
                    divisor = points[column_index] - points[other_index]
                    shifted = [0.0] + coeffs
                    widened = coeffs + [0.0]
                    coeffs = [
                        (shifted[place] - points[other_index] * widened[place]) / divisor
                        for place in range(len(shifted))
                    ]
            integral = 0.0
            for place in range(len(coeffs)):
                integral = integral + coeffs[place] * points[row_index] ** (place + 1) / (place + 1)
            entries.append(integral)
        quadrature.append(entries)
    return (points, quadrature)


def cas_table(length):
    indices = np.arange(length)
    phases = (indices[:, None] * indices[None, :] % length) * (2.0 * math.pi / length)
    return (np.cos(phases) + np.sin(phases)) / math.sqrt(length)


def eigen_line(length):
    return -4.0 * np.sin(np.arange(length) * (math.pi / length)) ** 2


def halves(table):
    high = table.astype(np.float32).astype(BF16)
    low = (table - high.astype(np.float64)).astype(np.float32).astype(BF16)
    return high, low


def tables():
    line = cas_table(CELLS)
    high, low = halves(line)
    right = np.concatenate([part for h in (slice(0, 128), slice(128, 256)) for part in (high[h], high[h], low[h])], 0)
    left = np.concatenate([high, high, low], 1)
    cas_x = cas_table(64)
    cross = np.zeros((2, 64, SLABS, 2, 4))
    for row in range(2):
        cross[row, :, :, row, :] = cas_x.reshape(64, SLABS, 4)
    cross = cross.reshape(128, 128)
    high, low = halves(cross)
    forward = np.concatenate([high, high, low], 1)
    high, low = halves(cross.T)
    back = np.concatenate([high, high, low], 1)
    lam_x = np.broadcast_to((STEP * eigen_line(64))[:, None], (64, 128)).astype(np.float32)
    lam_z = np.broadcast_to((STEP * eigen_line(CELLS)).reshape(2, 1, 128), (2, 8, 128)).astype(np.float32)
    lam_y = np.broadcast_to((STEP * eigen_line(CELLS)).reshape(DEVS, 2, 1), (DEVS, 2, 128)).astype(np.float32)
    return right, left, forward, back, lam_x, lam_z, lam_y


def split(value, axis):
    high = value.astype(BF16)
    low = (value - high.astype(F32)).astype(BF16)
    return jnp.concatenate([high, low, high], axis)


def split_halves(first, second):
    return jnp.concatenate([split(first, 1), split(second, 1)], 1)


def matmul(a, b):
    return jnp.dot(a, b, preferred_element_type=F32)


def kernel(
    points, quadrature,
    sec_hbm, ini_hbm, right_hbm, left_hbm, fwd_hbm, back_hbm, lam_x_hbm, lam_z_hbm, lam_y_hbm,
    first, last, peak,
    sec, ini, right, left, fwd, back, lam_x, lam_z, lam_y,
    rows, rows0, sent, sent0, got, got0, modes, modes0, spect, bsent, bgot, peak_sent, peak_got,
    in_sem, send_sem, send0_sem, got_sem, got0_sem, bsend_sem, bgot_sem, psend_sem, pgot_sem,
):
    here = tuple(lax.axis_index(a) for a in AXES)
    my_node = here[0] * 4 + here[1]
    my_slab = (here[2] * 4 + here[3]) * 2 + here[4]
    me = my_node * SLABS + my_slab
    my_y = here[0] * 2 + here[2]

    loads = [
        pltpu.make_async_copy(src, dst, in_sem.at[i])
        for i, (src, dst) in enumerate([
            (left_hbm, left), (sec_hbm.at[0], sec), (right_hbm, right), (ini_hbm, ini), (fwd_hbm, fwd),
            (back_hbm, back), (lam_x_hbm, lam_x), (lam_z_hbm, lam_z), (lam_y_hbm.at[me], lam_y),
        ])
    ]

    def flat(t):
        return (((t[0] * 4 + t[1]) * 2 + t[2]) * 4 + t[3]) * 2 + t[4]

    cores = (here[4], 1 - here[4])
    planes = [lax.rem(my_y + k, 4) for k in range(4)]
    planes = [(y // 2, lax.rem(y, 2)) for y in planes]
    across = [lax.rem(here[3] + k, 4) for k in range(4)]
    depths = [lax.rem(here[1] + k, 4) for k in range(4)]

    def far_first(visit, low=0, high=DEVS - 1):
        for y, z, x, core in FAR_FIRST[low:high]:
            visit((planes[y][0], depths[z], planes[y][1], across[x], cores[core]))

    barrier = pltpu.get_barrier_semaphore()

    far_first(lambda t: pl.semaphore_signal(barrier, inc=1, device_id=t, device_id_type=MESH))

    for load in loads:
        load.start()

    def put(buf, x, count, value):
        for h in range(2):
            buf[h, pl.ds(x, count, stride=4), :] = value[:, 128 * h : 128 * h + 128]

    loads[0].wait()
    loads[1].wait()
    for x in range(4):
        put(rows, x, CELLS, matmul(left[...], split(sec[x], 0)))
    loads[2].wait()
    for b in range(4):
        part = split_halves(*(rows[h, pl.ds(CELLS * b, CELLS), :] for h in range(2)))
        part = matmul(part, right[...])
        for h in range(2):
            sent[h, pl.ds(32 * b, 32)] = part[:, 128 * h : 128 * h + 128].reshape(32, 8, 128)
    pl.semaphore_wait(barrier, DEVS - 1)

    def spread(src, dst, s_sem, r_sem, low=0, high=DEVS - 1):
        far_first(
            lambda t: pltpu.make_async_remote_copy(
                src.at[flat(t)], dst.at[me], s_sem, r_sem, device_id=t, device_id_type=MESH
            ).start(),
            low, high,
        )
        if low == 0:
            dst[me] = src[me]

    def all_but_one(buf, count, sem):
        view = buf.at[pl.ds(0, count - 1)]
        pltpu.make_async_copy(view, view, sem).wait()

    spread(sent.at[0], got.at[0], send_sem.at[0], got_sem.at[0])
    loads[3].wait()
    mine = left[pl.ds(pl.multiple_of(my_node * 32, 32), 32), :]
    for x in range(4):
        put(rows0, x, 32, matmul(mine, split(ini[x], 0)))
    part = matmul(split_halves(rows0[0], rows0[1]), right[...])
    for h in range(2):
        sent0[h] = part[:, 128 * h : 128 * h + 128].reshape(16, 8, 128)

    for h in range(2):
        for k in range(1, SLABS):
            x = lax.rem(here[3] + k, 4)
            t = (here[0], here[1], here[2] if k < 8 else 1 - here[2], x, cores[k // 4 % 2])
            pltpu.make_async_remote_copy(
                sent0.at[h, (t[2] * 4 + t[3]) * 2 + t[4]], got0.at[h, my_slab], send0_sem.at[h], got0_sem.at[h],
                device_id=t, device_id_type=MESH,
            ).start()
        got0[h, my_slab] = sent0[h, my_slab]
    spread(sent.at[1], got.at[1], send_sem.at[1], got_sem.at[1])

    for load in loads[4:]:
        load.wait()

    def enter(h):
        all_but_one(got0.at[h], SLABS, got0_sem.at[h])
        all_but_one(got.at[h], DEVS, got_sem.at[h])
        modes0[...] = matmul(fwd[...], split(got0[h].reshape(128, 128), 0))
        for n in range(0, NODES, 2):
            pair = [got[h, pl.ds(SLABS * (n + k), SLABS)].reshape(128, 128) for k in range(2)]
            modes[:, 128 * n : 128 * n + 256] = matmul(fwd[...], split(jnp.concatenate(pair, 1), 0))

    def sweep(k, h):
        lam_0 = [lam_z[h] + lam_y[row : row + 1, :] for row in range(2)]

        def one(i, carry):
            lam_1 = lam_x[pl.ds(pl.multiple_of(8 * i, 8), 8), :]
            for row in range(2):
                r = pl.multiple_of(64 * row + 8 * i, 8)
                lam = lam_1 + lam_0[row]
                start = modes0[pl.ds(r, 8), :]
                value = [modes[pl.ds(r, 8), 128 * m : 128 * m + 128] for m in range(NODES)]
                slope = [lam * v for v in value]
                for m in range(NODES):
                    total = start - value[m]
                    for j in range(NODES):
                        total = total + quadrature[m][j] * slope[j]
                    spect[pl.ds(r, 8), 128 * m : 128 * m + 128] = total
                    modes[pl.ds(r, 8), 128 * m : 128 * m + 128] = value[m] + total / (
                        1.0 - (points[m] / (k + 1.0)) * lam
                    )
            return carry

        lax.fori_loop(0, 8, one, 0)

    def make(f, h):
        source = spect if f < SWEEPS else modes
        for n in range(0, NODES, 2):
            pair = matmul(back[...], split(source[:, 128 * n : 128 * n + 256], 0))
            for k in range(2):
                block = pair[:, 128 * k : 128 * k + 128]
                if f < SWEEPS:
                    bsent[f, h, pl.ds(SLABS * (n + k), SLABS)] = block.reshape(SLABS, 8, 128)
                else:
                    rows[h, pl.ds(128 * (n + k), 128), :] = block

    def make_z():
        for b in range(4):
            part = split_halves(*(rows[h, pl.ds(CELLS * b, CELLS), :] for h in range(2)))
            part = matmul(part, right[...])
            for h in range(2):
                bsent[SWEEPS, h, pl.ds(32 * b, 32)] = part[:, 128 * h : 128 * h + 128].reshape(32, 8, 128)

    def give(f, h, *how):
        spread(bsent.at[f, h], bgot.at[f, h], bsend_sem.at[f, h], bgot_sem.at[f, h], *how)

    enter(0)
    for f in range(FIELDS):
        if f < SWEEPS:
            sweep(f, 0)
        make(f, 0)
        if f < 2:
            give(f, 0)
    enter(1)
    for f in range(FIELDS):
        if f < SWEEPS:
            sweep(f, 1)
        make(f, 1)
        if f == SWEEPS:
            make_z()
        if f >= 2:
            give(f, 0)
        give(f, 1, *(() if f < SWEEPS else (0, 72)))

    def ready(f, h):
        all_but_one(bgot.at[f, h], DEVS, bgot_sem.at[f, h])

    def plane(f, h, x):
        return bgot.at[f, h].reshape(4 * CELLS, 128)[pl.ds(x, CELLS, stride=4), :]

    def pairs(h):
        for x in range(0, 4, 2):
            part = jnp.concatenate([plane(SWEEPS, h, x + k) for k in range(2)], 1)
            part = matmul(left[...], split(part, 0))
            yield x, part[:, :128]
            yield x + 1, part[:, 128:]

    lane = lax.broadcasted_iota(jnp.int32, (1, 128), 1)
    peaks = jnp.zeros((1, 128), F32)
    for f in range(SWEEPS):
        ready(f, 0)
        ready(f, 1)
        top = None
        for x in range(4):
            part = jnp.concatenate([plane(f, h, x) for h in range(2)], 1)
            part = matmul(left[...], split(part, 0))
            part = matmul(split_halves(part[:, :128], part[:, 128:]), right[...])
            part = jnp.max(jnp.abs(part).reshape(32, 8, CELLS), axis=0)
            top = part if top is None else jnp.maximum(top, part)
        peaks = jnp.where(lane == f, jnp.max(top), peaks)
    peak_sent[...] = peaks

    far_first(
        lambda t: pltpu.make_async_remote_copy(
            peak_sent, peak_got.at[me], psend_sem, pgot_sem, device_id=t, device_id_type=MESH
        ).start()
    )
    peak_got[me] = peaks
    give(SWEEPS, 1, 72, DEVS - 1)
    ready(SWEEPS, 0)
    for x, part in pairs(0):
        first[x] = part
    all_but_one(peak_got, DEVS, pgot_sem)
    peak[...] = jnp.max(peak_got[...], axis=0)
    for h in range(2):
        all_but_one(sent0.at[h], SLABS, send0_sem.at[h])
        all_but_one(sent.at[h], DEVS, send_sem.at[h])
        for f in range(FIELDS):
            all_but_one(bsent.at[f, h], DEVS, bsend_sem.at[f, h])
    all_but_one(peak_got, DEVS, psend_sem)
    ready(SWEEPS, 1)
    for x, part in pairs(1):
        last[x] = part


def finish(first, last, peak, out_hbm, res_hbm, res, out_sem):
    copies = [
        pltpu.make_async_copy(part, out_hbm.at[0, :, :, pl.ds(128 * h, 128)], out_sem.at[h])
        for h, part in enumerate((first, last))
    ]
    for copy in copies:
        copy.start()
    lane = lax.broadcasted_iota(jnp.int32, (1, 128), 1)
    for f in range(SWEEPS):
        res[f] = jnp.max(jnp.where(lane == f, peak[...], 0.0))
    copies.append(pltpu.make_async_copy(res, res_hbm, out_sem.at[2]))
    copies[2].start()
    for copy in copies:
        copy.wait()


def on_device(initial, sections):
    points, quadrature = radau_tables(NODES)
    any_space = pl.BlockSpec(memory_space=pl.ANY)
    dma = pltpu.SemaphoreType.DMA
    parts = [jnp.asarray(t) for t in tables()]
    vmem = pltpu.VMEM
    whole = pl.BlockSpec(memory_space=pltpu.VMEM)
    pinned = pl.BlockSpec(memory_space=pltpu.HBM)
    found = pl.pallas_call(
        functools.partial(kernel, points, quadrature),
        out_shape=(
            jax.ShapeDtypeStruct((4, CELLS, 128), F32),
            jax.ShapeDtypeStruct((4, CELLS, 128), F32),
            jax.ShapeDtypeStruct((1, 128), F32),
        ),
        in_specs=[pinned] * 9,
        out_specs=(whole,) * 3,
        scratch_shapes=[
            vmem((4, CELLS, CELLS), F32),
            vmem((4, CELLS, CELLS), F32),
            vmem((3 * CELLS, CELLS), BF16),
            vmem((CELLS, 3 * CELLS), BF16),
            vmem((128, 384), BF16),
            vmem((128, 384), BF16),
            vmem((64, 128), F32),
            vmem((2, 8, 128), F32),
            vmem((2, 128), F32),
            vmem((2, 4 * CELLS, 128), F32),
            vmem((2, 128, 128), F32),
            vmem((2, DEVS, 8, 128), F32),
            vmem((2, SLABS, 8, 128), F32),
            vmem((2, DEVS, 8, 128), F32),
            vmem((2, SLABS, 8, 128), F32),
            vmem((128, NODES * 128), F32),
            vmem((128, 128), F32),
            vmem((128, NODES * 128), F32),
            vmem((FIELDS, 2, DEVS, 8, 128), F32),
            vmem((FIELDS, 2, DEVS, 8, 128), F32),
            vmem((1, 128), F32),
            vmem((DEVS, 1, 128), F32),
            dma((9,)),
            dma((2,)),
            dma((2,)),
            dma((2,)),
            dma((2,)),
            dma((FIELDS, 2)),
            dma((FIELDS, 2)),
            dma,
            dma,
        ],
        compiler_params=pltpu.CompilerParams(
            collective_id=0, has_side_effects=True, vmem_limit_bytes=30 << 20
        ),
        name="sdc",
    )(*(pltpu.with_memory_space_constraint(value, pltpu.HBM) for value in (sections, initial, *parts)))
    return pl.pallas_call(
        finish,
        out_shape=(
            jax.ShapeDtypeStruct(sections.shape, F32),
            jax.ShapeDtypeStruct((SWEEPS,), F32),
        ),
        in_specs=[whole] * 3,
        out_specs=(any_space, any_space),
        scratch_shapes=[pltpu.SMEM((SWEEPS,), F32), dma((3,))],
        compiler_params=pltpu.CompilerParams(vmem_limit_bytes=16 << 20),
        name="finish",
    )(*found)


def solution(mesh):
    torus = Mesh(mesh.devices.reshape(2, 4, 2, 4, 2), AXES)
    return jax.shard_map(
        on_device,
        mesh=torus,
        in_specs=(P(SLAB, None, None), P(NODE, SLAB, None, None)),
        out_specs=(P(NODE, SLAB, None, None), P()),
        check_vma=False,
    )
```

```python
import functools
import math

import jax
import jax.numpy as jnp
import numpy as np
from jax import lax
from jax.experimental import pallas as pl
from jax.experimental.pallas import tpu as pltpu
from jax.sharding import Mesh
from jax.sharding import PartitionSpec as P

SWEEPS = 3
AXES = ("node_0", "node_1", "slab_0", "slab_1", "slab_2")
SLAB = ("slab_0", "slab_1", "slab_2")
NODE = ("node_0", "node_1")
MESH = pl.DeviceIdType.MESH
F32 = jnp.float32
BF16 = jnp.bfloat16
STEP = 4.0
NODES = 8
SLABS = 16
DEVS = NODES * SLABS
CELLS = 256
FIELDS = SWEEPS + 1
HOPS = (0, 1, 2, 1)
FAR_FIRST = sorted(
    ((k // 4 % 4, k % 4, (k + k // 16) % 4, k // 64) for k in (37 * j % DEVS for j in range(DEVS))),
    key=lambda offset: -sum(HOPS[step] for step in offset[:3]),
)
FAR_FIRST.remove((0, 0, 0, 0))


def radau_value(order, point):
    prev_value = 1.0
    prev_slope = 0.0
    this_value = point
    this_slope = 1.0
    for degree in range(1, order):
        next_value = ((2 * degree + 1) * point * this_value - degree * prev_value) / (degree + 1)
        next_slope = (
            (2 * degree + 1) * (this_value + point * this_slope) - degree * prev_slope
        ) / (degree + 1)
        prev_value, prev_slope = (this_value, this_slope)
        this_value, this_slope = (next_value, next_slope)
    return (this_value - prev_value, this_slope - prev_slope)


def radau_tables(node_total):
    points = []
    for node_index in range(node_total):
        estimate = math.cos(2.0 * math.pi * node_index / (2 * node_total - 1))
        if node_index > 0:
            for repeat in range(60):
                poly_value, poly_slope = radau_value(node_total, estimate)
                estimate = estimate - poly_value / poly_slope
        points.append((estimate + 1.0) / 2.0)
    points = sorted(points)
    quadrature = []
    for row_index in range(node_total):
        entries = []
        for column_index in range(node_total):
            coeffs = [1.0]
            for other_index in range(node_total):
                if other_index != column_index:
                    divisor = points[column_index] - points[other_index]
                    shifted = [0.0] + coeffs
                    widened = coeffs + [0.0]
                    coeffs = [
                        (shifted[place] - points[other_index] * widened[place]) / divisor
                        for place in range(len(shifted))
                    ]
            integral = 0.0
            for place in range(len(coeffs)):
                integral = integral + coeffs[place] * points[row_index] ** (place + 1) / (place + 1)
            entries.append(integral)
        quadrature.append(entries)
    return (points, quadrature)


def cas_table(length):
    indices = np.arange(length)
    phases = (indices[:, None] * indices[None, :] % length) * (2.0 * math.pi / length)
    return (np.cos(phases) + np.sin(phases)) / math.sqrt(length)


def eigen_line(length):
    return -4.0 * np.sin(np.arange(length) * (math.pi / length)) ** 2


def halves(table):
    high = table.astype(np.float32).astype(BF16)
    low = (table - high.astype(np.float64)).astype(np.float32).astype(BF16)
    return high, low


def tables():
    line = cas_table(CELLS)
    high, low = halves(line)
    right = np.concatenate([part for h in (slice(0, 128), slice(128, 256)) for part in (high[h], high[h], low[h])], 0)
    left = np.concatenate([high, high, low], 1)
    cas_x = cas_table(64)
    cross = np.zeros((2, 64, SLABS, 2, 4))
    for row in range(2):
        cross[row, :, :, row, :] = cas_x.reshape(64, SLABS, 4)
    cross = cross.reshape(128, 128)
    high, low = halves(cross)
    forward = np.concatenate([high, high, low], 1)
    high, low = halves(cross.T)
    back = np.concatenate([high, high, low], 1)
    lam_x = np.broadcast_to((STEP * eigen_line(64))[:, None], (64, 128)).astype(np.float32)
    lam_z = np.broadcast_to((STEP * eigen_line(CELLS)).reshape(2, 1, 128), (2, 8, 128)).astype(np.float32)
    lam_y = np.broadcast_to((STEP * eigen_line(CELLS)).reshape(DEVS, 2, 1), (DEVS, 2, 128)).astype(np.float32)
    return right, left, forward, back, lam_x, lam_z, lam_y


def split(value, axis):
    high = value.astype(BF16)
    low = (value - high.astype(F32)).astype(BF16)
    return jnp.concatenate([high, low, high], axis)


def split_halves(first, second):
    return jnp.concatenate([split(first, 1), split(second, 1)], 1)


def matmul(a, b):
    return jnp.dot(a, b, preferred_element_type=F32)


def kernel(
    points, quadrature,
    sec_hbm, ini_hbm, right_hbm, left_hbm, fwd_hbm, back_hbm, lam_x_hbm, lam_z_hbm, lam_y_hbm,
    first, last, peak,
    sec, ini, right, left, fwd, back, lam_x, lam_z, lam_y,
    rows, rows0, sent, sent0, got, got0, modes, modes0, spect, bsent, bgot, peak_sent, peak_got, peak_all,
    in_sem, send_sem, send0_sem, got_sem, got0_sem, bsend_sem, bgot_sem, psend_sem, pgot_sem,
):
    here = tuple(lax.axis_index(a) for a in AXES)
    my_node = here[0] * 4 + here[1]
    my_slab = (here[2] * 4 + here[3]) * 2 + here[4]
    me = my_node * SLABS + my_slab
    my_y = here[0] * 2 + here[2]

    loads = [
        pltpu.make_async_copy(src, dst, in_sem.at[i])
        for i, (src, dst) in enumerate([
            (left_hbm, left), (sec_hbm.at[0], sec), (right_hbm, right), (ini_hbm, ini), (fwd_hbm, fwd),
            (back_hbm, back), (lam_x_hbm, lam_x), (lam_z_hbm, lam_z), (lam_y_hbm.at[me], lam_y),
        ])
    ]

    def flat(t):
        return (((t[0] * 4 + t[1]) * 2 + t[2]) * 4 + t[3]) * 2 + t[4]

    cores = (here[4], 1 - here[4])
    planes = [lax.rem(my_y + k, 4) for k in range(4)]
    planes = [(y // 2, lax.rem(y, 2)) for y in planes]
    across = [lax.rem(here[3] + k, 4) for k in range(4)]
    depths = [lax.rem(here[1] + k, 4) for k in range(4)]

    def far_first(visit):
        for y, z, x, core in FAR_FIRST:
            visit((planes[y][0], depths[z], planes[y][1], across[x], cores[core]))

    barrier = pltpu.get_barrier_semaphore()

    far_first(lambda t: pl.semaphore_signal(barrier, inc=1, device_id=t, device_id_type=MESH))

    for load in loads:
        load.start()

    def put(buf, x, count, value):
        for h in range(2):
            buf[h, pl.ds(x, count, stride=4), :] = value[:, 128 * h : 128 * h + 128]

    loads[0].wait()
    loads[1].wait()
    for x in range(4):
        put(rows.at[0], x, CELLS, matmul(left[...], split(sec[x], 0)))
    loads[2].wait()
    for b in range(4):
        part = split_halves(*(rows[0, h, pl.ds(CELLS * b, CELLS), :] for h in range(2)))
        part = matmul(part, right[...])
        for h in range(2):
            sent[h, pl.ds(32 * b, 32)] = part[:, 128 * h : 128 * h + 128].reshape(32, 8, 128)
    pl.semaphore_wait(barrier, DEVS - 1)

    def spread(src, dst, s_sem, r_sem):
        far_first(
            lambda t: pltpu.make_async_remote_copy(
                src.at[flat(t)], dst.at[me], s_sem, r_sem, device_id=t, device_id_type=MESH
            ).start()
        )
        dst[me] = src[me]

    def all_but_one(buf, count, sem):
        view = buf.at[pl.ds(0, count - 1)]
        pltpu.make_async_copy(view, view, sem).wait()

    spread(sent.at[0], got.at[0], send_sem.at[0], got_sem.at[0])
    loads[3].wait()
    mine = left[pl.ds(pl.multiple_of(my_node * 32, 32), 32), :]
    for x in range(4):
        put(rows0, x, 32, matmul(mine, split(ini[x], 0)))
    part = matmul(split_halves(rows0[0], rows0[1]), right[...])
    for h in range(2):
        sent0[h] = part[:, 128 * h : 128 * h + 128].reshape(16, 8, 128)

    for h in range(2):
        for k in range(1, SLABS):
            x = lax.rem(here[3] + k, 4)
            t = (here[0], here[1], here[2] if k < 8 else 1 - here[2], x, cores[k // 4 % 2])
            pltpu.make_async_remote_copy(
                sent0.at[h, (t[2] * 4 + t[3]) * 2 + t[4]], got0.at[h, my_slab], send0_sem.at[h], got0_sem.at[h],
                device_id=t, device_id_type=MESH,
            ).start()
        got0[h, my_slab] = sent0[h, my_slab]
    spread(sent.at[1], got.at[1], send_sem.at[1], got_sem.at[1])

    for load in loads[4:]:
        load.wait()

    def enter(h):
        all_but_one(got0.at[h], SLABS, got0_sem.at[h])
        all_but_one(got.at[h], DEVS, got_sem.at[h])
        modes0[...] = matmul(fwd[...], split(got0[h].reshape(128, 128), 0))
        for n in range(0, NODES, 2):
            pair = [got[h, pl.ds(SLABS * (n + k), SLABS)].reshape(128, 128) for k in range(2)]
            modes[:, 128 * n : 128 * n + 256] = matmul(fwd[...], split(jnp.concatenate(pair, 1), 0))

    def sweep(k, h):
        lam_0 = [lam_z[h] + lam_y[row : row + 1, :] for row in range(2)]

        def one(i, carry):
            lam_1 = lam_x[pl.ds(pl.multiple_of(8 * i, 8), 8), :]
            for row in range(2):
                r = pl.multiple_of(64 * row + 8 * i, 8)
                lam = lam_1 + lam_0[row]
                start = modes0[pl.ds(r, 8), :]
                value = [modes[pl.ds(r, 8), 128 * m : 128 * m + 128] for m in range(NODES)]
                slope = [lam * v for v in value]
                for m in range(NODES):
                    total = start - value[m]
                    for j in range(NODES):
                        total = total + quadrature[m][j] * slope[j]
                    spect[pl.ds(r, 8), 128 * m : 128 * m + 128] = total
                    modes[pl.ds(r, 8), 128 * m : 128 * m + 128] = value[m] + total / (
                        1.0 - (points[m] / (k + 1.0)) * lam
                    )
            return carry

        lax.fori_loop(0, 8, one, 0)

    def make(f, h):
        source = spect if f < SWEEPS else modes
        for n in range(0, NODES, 2):
            pair = matmul(back[...], split(source[:, 128 * n : 128 * n + 256], 0))
            for k in range(2):
                block = pair[:, 128 * k : 128 * k + 128]
                if f < 2:
                    bsent[f, h, pl.ds(SLABS * (n + k), SLABS)] = block.reshape(SLABS, 8, 128)
                else:
                    rows[f - 2, h, pl.ds(128 * (n + k), 128), :] = block

    def make_z(f):
        for b in range(4):
            part = split_halves(*(rows[f - 2, h, pl.ds(CELLS * b, CELLS), :] for h in range(2)))
            part = matmul(part, right[...])
            for h in range(2):
                bsent[f, h, pl.ds(32 * b, 32)] = part[:, 128 * h : 128 * h + 128].reshape(32, 8, 128)

    def give(f, h):
        spread(bsent.at[f, h], bgot.at[f, h], bsend_sem.at[f, h], bgot_sem.at[f, h])

    enter(0)
    for f in range(FIELDS):
        if f < SWEEPS:
            sweep(f, 0)
        make(f, 0)
        if f < 2:
            give(f, 0)
    enter(1)
    for f in range(FIELDS):
        if f < SWEEPS:
            sweep(f, 1)
        make(f, 1)
        if f >= 2:
            make_z(f)
            give(f, 0)
        if f < SWEEPS:
            give(f, 1)

    def ready(f, h):
        all_but_one(bgot.at[f, h], DEVS, bgot_sem.at[f, h])

    def plane(f, h, x):
        return bgot.at[f, h].reshape(4 * CELLS, 128)[pl.ds(x, CELLS, stride=4), :]

    def pairs(f, h):
        for x in range(0, 4, 2):
            part = jnp.concatenate([plane(f, h, x + k) for k in range(2)], 1)
            part = matmul(left[...], split(part, 0))
            yield x, part[:, :128]
            yield x + 1, part[:, 128:]

    def peak_of(parts):
        parts = [jnp.max(jnp.abs(part).reshape(32, 8, part.shape[1]), axis=0) for part in parts]
        return jnp.max(functools.reduce(jnp.maximum, parts))

    lane = lax.broadcasted_iota(jnp.int32, (1, 128), 1)
    peaks = jnp.zeros((1, 128), F32)
    for f in range(2):
        ready(f, 0)
        ready(f, 1)
        parts = []
        for x in range(4):
            part = jnp.concatenate([plane(f, h, x) for h in range(2)], 1)
            part = matmul(left[...], split(part, 0))
            parts.append(matmul(split_halves(part[:, :128], part[:, 128:]), right[...]))
        peaks = jnp.where(lane == f, peak_of(parts), peaks)
    for h in range(2):
        ready(2, h)
        top = peak_of([part for x, part in pairs(2, h)])
        peaks = jnp.maximum(peaks, jnp.where(lane == 2, top, 0.0))
    peak_sent[0] = peaks

    place = here[1] * 4 + here[3]
    for k in range(1, 16):
        pltpu.make_async_remote_copy(
            peak_sent.at[0], peak_got.at[place], psend_sem.at[0], pgot_sem.at[0],
            device_id=(here[0], depths[k // 4], here[2], across[k % 4], here[4]), device_id_type=MESH,
        ).start()
    peak_got[place] = peaks
    give(SWEEPS, 1)
    ready(SWEEPS, 0)
    for x, part in pairs(SWEEPS, 0):
        first[x] = part
    all_but_one(peak_got, 16, pgot_sem.at[0])
    peaks = jnp.max(peak_got[...], axis=0)
    peak_sent[1] = peaks
    place = my_y * 2 + here[4]
    for k in range(1, 8):
        pltpu.make_async_remote_copy(
            peak_sent.at[1], peak_all.at[place], psend_sem.at[1], pgot_sem.at[1],
            device_id=(planes[k // 2][0], here[1], planes[k // 2][1], here[3], cores[k % 2]),
            device_id_type=MESH,
        ).start()
    peak_all[place] = peaks
    all_but_one(peak_all, 8, pgot_sem.at[1])
    peak[...] = jnp.max(peak_all[...], axis=0)
    for h in range(2):
        all_but_one(sent0.at[h], SLABS, send0_sem.at[h])
        all_but_one(sent.at[h], DEVS, send_sem.at[h])
        for f in range(FIELDS):
            all_but_one(bsent.at[f, h], DEVS, bsend_sem.at[f, h])
    all_but_one(peak_got, 16, psend_sem.at[0])
    all_but_one(peak_all, 8, psend_sem.at[1])
    ready(SWEEPS, 1)
    for x, part in pairs(SWEEPS, 1):
        last[x] = part


def finish(first, last, peak, out_hbm, res_hbm, res, out_sem):
    copies = [
        pltpu.make_async_copy(part, out_hbm.at[0, :, :, pl.ds(128 * h, 128)], out_sem.at[h])
        for h, part in enumerate((first, last))
    ]
    for copy in copies:
        copy.start()
    lane = lax.broadcasted_iota(jnp.int32, (1, 128), 1)
    for f in range(SWEEPS):
        res[f] = jnp.max(jnp.where(lane == f, peak[...], 0.0))
    copies.append(pltpu.make_async_copy(res, res_hbm, out_sem.at[2]))
    copies[2].start()
    for copy in copies:
        copy.wait()


def on_device(initial, sections):
    points, quadrature = radau_tables(NODES)
    any_space = pl.BlockSpec(memory_space=pl.ANY)
    dma = pltpu.SemaphoreType.DMA
    parts = [jnp.asarray(t) for t in tables()]
    vmem = pltpu.VMEM
    whole = pl.BlockSpec(memory_space=pltpu.VMEM)
    pinned = pl.BlockSpec(memory_space=pltpu.HBM)
    found = pl.pallas_call(
        functools.partial(kernel, points, quadrature),
        out_shape=(
            jax.ShapeDtypeStruct((4, CELLS, 128), F32),
            jax.ShapeDtypeStruct((4, CELLS, 128), F32),
            jax.ShapeDtypeStruct((1, 128), F32),
        ),
        in_specs=[pinned] * 9,
        out_specs=(whole,) * 3,
        scratch_shapes=[
            vmem((4, CELLS, CELLS), F32),
            vmem((4, CELLS, CELLS), F32),
            vmem((3 * CELLS, CELLS), BF16),
            vmem((CELLS, 3 * CELLS), BF16),
            vmem((128, 384), BF16),
            vmem((128, 384), BF16),
            vmem((64, 128), F32),
            vmem((2, 8, 128), F32),
            vmem((2, 128), F32),
            vmem((2, 2, 4 * CELLS, 128), F32),
            vmem((2, 128, 128), F32),
            vmem((2, DEVS, 8, 128), F32),
            vmem((2, SLABS, 8, 128), F32),
            vmem((2, DEVS, 8, 128), F32),
            vmem((2, SLABS, 8, 128), F32),
            vmem((128, NODES * 128), F32),
            vmem((128, 128), F32),
            vmem((128, NODES * 128), F32),
            vmem((FIELDS, 2, DEVS, 8, 128), F32),
            vmem((FIELDS, 2, DEVS, 8, 128), F32),
            vmem((2, 1, 128), F32),
            vmem((16, 1, 128), F32),
            vmem((8, 1, 128), F32),
            dma((9,)),
            dma((2,)),
            dma((2,)),
            dma((2,)),
            dma((2,)),
            dma((FIELDS, 2)),
            dma((FIELDS, 2)),
            dma((2,)),
            dma((2,)),
        ],
        compiler_params=pltpu.CompilerParams(
            collective_id=0, has_side_effects=True, vmem_limit_bytes=30 << 20
        ),
        name="sdc",
    )(*(pltpu.with_memory_space_constraint(value, pltpu.HBM) for value in (sections, initial, *parts)))
    return pl.pallas_call(
        finish,
        out_shape=(
            jax.ShapeDtypeStruct(sections.shape, F32),
            jax.ShapeDtypeStruct((SWEEPS,), F32),
        ),
        in_specs=[whole] * 3,
        out_specs=(any_space, any_space),
        scratch_shapes=[pltpu.SMEM((SWEEPS,), F32), dma((3,))],
        compiler_params=pltpu.CompilerParams(vmem_limit_bytes=16 << 20),
        name="finish",
    )(*found)


def solution(mesh):
    torus = Mesh(mesh.devices.reshape(2, 4, 2, 4, 2), AXES)
    return jax.shard_map(
        on_device,
        mesh=torus,
        in_specs=(P(SLAB, None, None), P(NODE, SLAB, None, None)),
        out_specs=(P(NODE, SLAB, None, None), P()),
        check_vma=False,
    )
```

```python
import functools
import math

import jax
import jax.numpy as jnp
import numpy as np
from jax import lax
from jax.experimental import pallas as pl
from jax.experimental.pallas import tpu as pltpu
from jax.sharding import Mesh
from jax.sharding import PartitionSpec as P

SWEEPS = 3
AXES = ("node_0", "node_1", "slab_0", "slab_1", "slab_2")
SLAB = ("slab_0", "slab_1", "slab_2")
NODE = ("node_0", "node_1")
MESH = pl.DeviceIdType.MESH
F32 = jnp.float32
BF16 = jnp.bfloat16
STEP = 4.0
NODES = 8
SLABS = 16
DEVS = NODES * SLABS
CELLS = 256
FIELDS = SWEEPS + 1
HOPS = (0, 1, 2, 1)
FAR_FIRST = sorted(
    ((k // 4 % 4, k % 4, (k + k // 16) % 4, k // 64) for k in (37 * j % DEVS for j in range(DEVS))),
    key=lambda offset: -sum(HOPS[step] for step in offset[:3]),
)
FAR_FIRST.remove((0, 0, 0, 0))


def radau_value(order, point):
    prev_value = 1.0
    prev_slope = 0.0
    this_value = point
    this_slope = 1.0
    for degree in range(1, order):
        next_value = ((2 * degree + 1) * point * this_value - degree * prev_value) / (degree + 1)
        next_slope = (
            (2 * degree + 1) * (this_value + point * this_slope) - degree * prev_slope
        ) / (degree + 1)
        prev_value, prev_slope = (this_value, this_slope)
        this_value, this_slope = (next_value, next_slope)
    return (this_value - prev_value, this_slope - prev_slope)


def radau_tables(node_total):
    points = []
    for node_index in range(node_total):
        estimate = math.cos(2.0 * math.pi * node_index / (2 * node_total - 1))
        if node_index > 0:
            for repeat in range(60):
                poly_value, poly_slope = radau_value(node_total, estimate)
                estimate = estimate - poly_value / poly_slope
        points.append((estimate + 1.0) / 2.0)
    points = sorted(points)
    quadrature = []
    for row_index in range(node_total):
        entries = []
        for column_index in range(node_total):
            coeffs = [1.0]
            for other_index in range(node_total):
                if other_index != column_index:
                    divisor = points[column_index] - points[other_index]
                    shifted = [0.0] + coeffs
                    widened = coeffs + [0.0]
                    coeffs = [
                        (shifted[place] - points[other_index] * widened[place]) / divisor
                        for place in range(len(shifted))
                    ]
            integral = 0.0
            for place in range(len(coeffs)):
                integral = integral + coeffs[place] * points[row_index] ** (place + 1) / (place + 1)
            entries.append(integral)
        quadrature.append(entries)
    return (points, quadrature)


def cas_table(length):
    indices = np.arange(length)
    phases = (indices[:, None] * indices[None, :] % length) * (2.0 * math.pi / length)
    return (np.cos(phases) + np.sin(phases)) / math.sqrt(length)


def eigen_line(length):
    return -4.0 * np.sin(np.arange(length) * (math.pi / length)) ** 2


def pieces(table):
    found = []
    for k in range(3):
        found.append(table.astype(np.float32).astype(BF16))
        table = table - found[-1].astype(np.float64)
    return found


def tables():
    line = cas_table(CELLS)
    parts = pieces(line)
    right = np.concatenate([part[h] for h in (slice(0, 128), slice(128, 256)) for part in parts], 0)
    left = np.concatenate(parts, 1)
    cas_x = cas_table(64)
    cross = np.zeros((2, 64, SLABS, 2, 4))
    for row in range(2):
        cross[row, :, :, row, :] = cas_x.reshape(64, SLABS, 4)
    cross = cross.reshape(128, 128)
    forward = np.concatenate(pieces(cross), 1)
    back = np.concatenate(pieces(cross.T), 1)
    lam_x = np.broadcast_to((STEP * eigen_line(64))[:, None], (64, 128)).astype(np.float32)
    lam_z = np.broadcast_to((STEP * eigen_line(CELLS)).reshape(2, 1, 128), (2, 8, 128)).astype(np.float32)
    lam_y = np.broadcast_to((STEP * eigen_line(CELLS)).reshape(DEVS, 2, 1), (DEVS, 2, 128)).astype(np.float32)
    return right, left, forward, back, lam_x, lam_z, lam_y


def split(value, axis):
    high = value.astype(BF16)
    low = (value - high.astype(F32)).astype(BF16)
    return jnp.concatenate([high, low, high], axis)


def split_fine(value, axis):
    high = value.astype(BF16)
    value = value - high.astype(F32)
    mid = value.astype(BF16)
    low = (value - mid.astype(F32)).astype(BF16)
    return jnp.concatenate([high, high, mid, high, mid, low], axis)


ROUGH = (0, 0, 1)
FINE = (0, 1, 0, 2, 1, 0)


def across(ref, order, width, rows=slice(None)):
    return jnp.concatenate([ref[rows, width * k : width * k + width] for k in order], 1)


def down(ref, order):
    return jnp.concatenate([ref[384 * h + 128 * k : 384 * h + 128 * k + 128, :] for h in range(2) for k in order], 0)


def split_halves(first, second):
    return jnp.concatenate([split(first, 1), split(second, 1)], 1)


def matmul(a, b):
    return jnp.dot(a, b, preferred_element_type=F32)


def kernel(
    points, quadrature,
    sec_hbm, ini_hbm, right_hbm, left_hbm, fwd_hbm, back_hbm, lam_x_hbm, lam_z_hbm, lam_y_hbm,
    first, last, peak,
    sec, ini, right, left, fwd, back, lam_x, lam_z, lam_y,
    rows, rows0, sent, sent0, got, got0, modes, modes0, spect, bsent, bgot, peak_sent, peak_got, peak_all,
    in_sem, send_sem, send0_sem, got_sem, got0_sem, bsend_sem, bgot_sem, psend_sem, pgot_sem,
):
    here = tuple(lax.axis_index(a) for a in AXES)
    my_node = here[0] * 4 + here[1]
    my_slab = (here[2] * 4 + here[3]) * 2 + here[4]
    me = my_node * SLABS + my_slab
    my_y = here[0] * 2 + here[2]

    loads = [
        pltpu.make_async_copy(src, dst, in_sem.at[i])
        for i, (src, dst) in enumerate([
            (left_hbm, left), (sec_hbm.at[0], sec), (right_hbm, right), (ini_hbm, ini), (fwd_hbm, fwd),
            (back_hbm, back), (lam_x_hbm, lam_x), (lam_z_hbm, lam_z), (lam_y_hbm.at[me], lam_y),
        ])
    ]

    def flat(t):
        return (((t[0] * 4 + t[1]) * 2 + t[2]) * 4 + t[3]) * 2 + t[4]

    cores = (here[4], 1 - here[4])
    planes = [lax.rem(my_y + k, 4) for k in range(4)]
    planes = [(y // 2, lax.rem(y, 2)) for y in planes]
    widths = [lax.rem(here[3] + k, 4) for k in range(4)]
    depths = [lax.rem(here[1] + k, 4) for k in range(4)]

    def far_first(visit):
        for y, z, x, core in FAR_FIRST:
            visit((planes[y][0], depths[z], planes[y][1], widths[x], cores[core]))

    barrier = pltpu.get_barrier_semaphore()

    for load in loads:
        load.start()
    far_first(lambda t: pl.semaphore_signal(barrier, inc=1, device_id=t, device_id_type=MESH))

    def put(buf, x, count, value):
        for h in range(2):
            buf[h, pl.ds(x, count, stride=4), :] = value[:, 128 * h : 128 * h + 128]

    loads[0].wait()
    loads[1].wait()
    for x in range(4):
        put(rows.at[0], x, CELLS, matmul(across(left, FINE, CELLS), split_fine(sec[x], 0)))
    loads[2].wait()
    for b in range(4):
        part = [split_fine(rows[0, h, pl.ds(CELLS * b, CELLS), :], 1) for h in range(2)]
        part = matmul(jnp.concatenate(part, 1), down(right, FINE))
        for h in range(2):
            sent[h, pl.ds(32 * b, 32)] = part[:, 128 * h : 128 * h + 128].reshape(32, 8, 128)
    pl.semaphore_wait(barrier, DEVS - 1)

    def spread(src, dst, s_sem, r_sem):
        far_first(
            lambda t: pltpu.make_async_remote_copy(
                src.at[flat(t)], dst.at[me], s_sem, r_sem, device_id=t, device_id_type=MESH
            ).start()
        )
        dst[me] = src[me]

    def all_but_one(buf, count, sem):
        view = buf.at[pl.ds(0, count - 1)]
        pltpu.make_async_copy(view, view, sem).wait()

    spread(sent.at[0], got.at[0], send_sem.at[0], got_sem.at[0])
    loads[3].wait()
    mine = across(left, FINE, CELLS, pl.ds(pl.multiple_of(my_node * 32, 32), 32))
    for x in range(4):
        put(rows0, x, 32, matmul(mine, split_fine(ini[x], 0)))
    part = jnp.concatenate([split_fine(rows0[h], 1) for h in range(2)], 1)
    part = matmul(part, down(right, FINE))
    for h in range(2):
        sent0[h] = part[:, 128 * h : 128 * h + 128].reshape(16, 8, 128)

    for h in range(2):
        for k in range(1, SLABS):
            x = lax.rem(here[3] + k, 4)
            t = (here[0], here[1], here[2] if k < 8 else 1 - here[2], x, cores[k // 4 % 2])
            pltpu.make_async_remote_copy(
                sent0.at[h, (t[2] * 4 + t[3]) * 2 + t[4]], got0.at[h, my_slab], send0_sem.at[h], got0_sem.at[h],
                device_id=t, device_id_type=MESH,
            ).start()
        got0[h, my_slab] = sent0[h, my_slab]
    spread(sent.at[1], got.at[1], send_sem.at[1], got_sem.at[1])

    for load in loads[4:]:
        load.wait()

    def enter(h):
        all_but_one(got0.at[h], SLABS, got0_sem.at[h])
        all_but_one(got.at[h], DEVS, got_sem.at[h])
        modes0[...] = matmul(across(fwd, FINE, 128), split_fine(got0[h].reshape(128, 128), 0))
        for n in range(0, NODES, 2):
            pair = [got[h, pl.ds(SLABS * (n + k), SLABS)].reshape(128, 128) for k in range(2)]
            modes[:, 128 * n : 128 * n + 256] = matmul(across(fwd, FINE, 128), split_fine(jnp.concatenate(pair, 1), 0))

    def sweep(k, h):
        lam_0 = [lam_z[h] + lam_y[row : row + 1, :] for row in range(2)]

        def one(i, carry):
            lam_1 = lam_x[pl.ds(pl.multiple_of(8 * i, 8), 8), :]
            for row in range(2):
                r = pl.multiple_of(64 * row + 8 * i, 8)
                lam = lam_1 + lam_0[row]
                start = modes0[pl.ds(r, 8), :]
                value = [modes[pl.ds(r, 8), 128 * m : 128 * m + 128] for m in range(NODES)]
                slope = [lam * v for v in value]
                for m in range(NODES):
                    total = start - value[m]
                    for j in range(NODES):
                        total = total + quadrature[m][j] * slope[j]
                    spect[pl.ds(r, 8), 128 * m : 128 * m + 128] = total
                    modes[pl.ds(r, 8), 128 * m : 128 * m + 128] = value[m] + total / (
                        1.0 - (points[m] / (k + 1.0)) * lam
                    )
            return carry

        lax.fori_loop(0, 8, one, 0)

    def make(f, h):
        source = spect if f < SWEEPS else modes
        for n in range(0, NODES, 2):
            pair = matmul(across(back, ROUGH, 128), split(source[:, 128 * n : 128 * n + 256], 0))
            for k in range(2):
                block = pair[:, 128 * k : 128 * k + 128]
                if f < 2:
                    bsent[f, h, pl.ds(SLABS * (n + k), SLABS)] = block.reshape(SLABS, 8, 128)
                else:
                    rows[f - 2, h, pl.ds(128 * (n + k), 128), :] = block

    def make_z(f):
        for b in range(4):
            part = split_halves(*(rows[f - 2, h, pl.ds(CELLS * b, CELLS), :] for h in range(2)))
            part = matmul(part, down(right, ROUGH))
            for h in range(2):
                bsent[f, h, pl.ds(32 * b, 32)] = part[:, 128 * h : 128 * h + 128].reshape(32, 8, 128)

    def give(f, h):
        spread(bsent.at[f, h], bgot.at[f, h], bsend_sem.at[f, h], bgot_sem.at[f, h])

    enter(0)
    for f in range(FIELDS):
        if f < SWEEPS:
            sweep(f, 0)
        make(f, 0)
        if f < 2:
            give(f, 0)
    enter(1)
    for f in range(FIELDS):
        if f < SWEEPS:
            sweep(f, 1)
        make(f, 1)
        if f >= 2:
            make_z(f)
            give(f, 0)
        if f < SWEEPS:
            give(f, 1)

    def ready(f, h):
        all_but_one(bgot.at[f, h], DEVS, bgot_sem.at[f, h])

    def plane(f, h, x):
        return bgot.at[f, h].reshape(4 * CELLS, 128)[pl.ds(x, CELLS, stride=4), :]

    def pairs(f, h):
        for x in range(0, 4, 2):
            part = jnp.concatenate([plane(f, h, x + k) for k in range(2)], 1)
            part = matmul(across(left, ROUGH, CELLS), split(part, 0))
            yield x, part[:, :128]
            yield x + 1, part[:, 128:]

    def peak_of(parts):
        parts = [jnp.max(jnp.abs(part).reshape(32, 8, part.shape[1]), axis=0) for part in parts]
        return jnp.max(functools.reduce(jnp.maximum, parts))

    lane = lax.broadcasted_iota(jnp.int32, (1, 128), 1)
    peaks = jnp.zeros((1, 128), F32)
    for f in range(2):
        ready(f, 0)
        ready(f, 1)
        parts = []
        for x in range(4):
            part = jnp.concatenate([plane(f, h, x) for h in range(2)], 1)
            part = matmul(across(left, ROUGH, CELLS), split(part, 0))
            parts.append(matmul(split_halves(part[:, :128], part[:, 128:]), down(right, ROUGH)))
        peaks = jnp.where(lane == f, peak_of(parts), peaks)
    for h in range(2):
        ready(2, h)
        top = peak_of([part for x, part in pairs(2, h)])
        peaks = jnp.maximum(peaks, jnp.where(lane == 2, top, 0.0))
    peak_sent[0] = peaks

    place = here[1] * 4 + here[3]
    for k in range(1, 16):
        pltpu.make_async_remote_copy(
            peak_sent.at[0], peak_got.at[place], psend_sem.at[0], pgot_sem.at[0],
            device_id=(here[0], depths[k // 4], here[2], widths[k % 4], here[4]), device_id_type=MESH,
        ).start()
    peak_got[place] = peaks
    give(SWEEPS, 1)
    ready(SWEEPS, 0)
    for x, part in pairs(SWEEPS, 0):
        first[x] = part
    all_but_one(peak_got, 16, pgot_sem.at[0])
    peaks = jnp.max(peak_got[...], axis=0)
    peak_sent[1] = peaks
    place = my_y * 2 + here[4]
    for k in range(1, 8):
        pltpu.make_async_remote_copy(
            peak_sent.at[1], peak_all.at[place], psend_sem.at[1], pgot_sem.at[1],
            device_id=(planes[k // 2][0], here[1], planes[k // 2][1], here[3], cores[k % 2]),
            device_id_type=MESH,
        ).start()
    peak_all[place] = peaks
    all_but_one(peak_all, 8, pgot_sem.at[1])
    peak[...] = jnp.max(peak_all[...], axis=0)
    for h in range(2):
        all_but_one(sent0.at[h], SLABS, send0_sem.at[h])
        all_but_one(sent.at[h], DEVS, send_sem.at[h])
        for f in range(FIELDS):
            all_but_one(bsent.at[f, h], DEVS, bsend_sem.at[f, h])
    all_but_one(peak_got, 16, psend_sem.at[0])
    all_but_one(peak_all, 8, psend_sem.at[1])
    ready(SWEEPS, 1)
    for x, part in pairs(SWEEPS, 1):
        last[x] = part


def finish(first, last, peak, out_hbm, res_hbm, res, out_sem):
    copies = [
        pltpu.make_async_copy(part, out_hbm.at[0, :, :, pl.ds(128 * h, 128)], out_sem.at[h])
        for h, part in enumerate((first, last))
    ]
    for copy in copies:
        copy.start()
    lane = lax.broadcasted_iota(jnp.int32, (1, 128), 1)
    for f in range(SWEEPS):
        res[f] = jnp.max(jnp.where(lane == f, peak[...], 0.0))
    copies.append(pltpu.make_async_copy(res, res_hbm, out_sem.at[2]))
    copies[2].start()
    for copy in copies:
        copy.wait()


def on_device(initial, sections):
    points, quadrature = radau_tables(NODES)
    any_space = pl.BlockSpec(memory_space=pl.ANY)
    dma = pltpu.SemaphoreType.DMA
    parts = [jnp.asarray(t) for t in tables()]
    vmem = pltpu.VMEM
    whole = pl.BlockSpec(memory_space=pltpu.VMEM)
    pinned = pl.BlockSpec(memory_space=pltpu.HBM)
    found = pl.pallas_call(
        functools.partial(kernel, points, quadrature),
        out_shape=(
            jax.ShapeDtypeStruct((4, CELLS, 128), F32),
            jax.ShapeDtypeStruct((4, CELLS, 128), F32),
            jax.ShapeDtypeStruct((1, 128), F32),
        ),
        in_specs=[pinned] * 9,
        out_specs=(whole,) * 3,
        scratch_shapes=[
            vmem((4, CELLS, CELLS), F32),
            vmem((4, CELLS, CELLS), F32),
            vmem((3 * CELLS, CELLS), BF16),
            vmem((CELLS, 3 * CELLS), BF16),
            vmem((128, 384), BF16),
            vmem((128, 384), BF16),
            vmem((64, 128), F32),
            vmem((2, 8, 128), F32),
            vmem((2, 128), F32),
            vmem((2, 2, 4 * CELLS, 128), F32),
            vmem((2, 128, 128), F32),
            vmem((2, DEVS, 8, 128), F32),
            vmem((2, SLABS, 8, 128), F32),
            vmem((2, DEVS, 8, 128), F32),
            vmem((2, SLABS, 8, 128), F32),
            vmem((128, NODES * 128), F32),
            vmem((128, 128), F32),
            vmem((128, NODES * 128), F32),
            vmem((FIELDS, 2, DEVS, 8, 128), F32),
            vmem((FIELDS, 2, DEVS, 8, 128), F32),
            vmem((2, 1, 128), F32),
            vmem((16, 1, 128), F32),
            vmem((8, 1, 128), F32),
            dma((9,)),
            dma((2,)),
            dma((2,)),
            dma((2,)),
            dma((2,)),
            dma((FIELDS, 2)),
            dma((FIELDS, 2)),
            dma((2,)),
            dma((2,)),
        ],
        compiler_params=pltpu.CompilerParams(
            collective_id=0, has_side_effects=True, vmem_limit_bytes=30 << 20
        ),
        name="sdc",
    )(*(pltpu.with_memory_space_constraint(value, pltpu.HBM) for value in (sections, initial, *parts)))
    return pl.pallas_call(
        finish,
        out_shape=(
            jax.ShapeDtypeStruct(sections.shape, F32),
            jax.ShapeDtypeStruct((SWEEPS,), F32),
        ),
        in_specs=[whole] * 3,
        out_specs=(any_space, any_space),
        scratch_shapes=[pltpu.SMEM((SWEEPS,), F32), dma((3,))],
        compiler_params=pltpu.CompilerParams(vmem_limit_bytes=16 << 20),
        name="finish",
    )(*found)


def solution(mesh):
    torus = Mesh(mesh.devices.reshape(2, 4, 2, 4, 2), AXES)
    return jax.shard_map(
        on_device,
        mesh=torus,
        in_specs=(P(SLAB, None, None), P(NODE, SLAB, None, None)),
        out_specs=(P(NODE, SLAB, None, None), P()),
        check_vma=False,
    )
```

```python
import functools
import math

import jax
import jax.numpy as jnp
import numpy as np
from jax import lax
from jax.experimental import pallas as pl
from jax.experimental.pallas import tpu as pltpu
from jax.sharding import Mesh
from jax.sharding import PartitionSpec as P

SWEEPS = 3
AXES = ("node_0", "node_1", "slab_0", "slab_1", "slab_2")
SLAB = ("slab_0", "slab_1", "slab_2")
NODE = ("node_0", "node_1")
MESH = pl.DeviceIdType.MESH
F32 = jnp.float32
BF16 = jnp.bfloat16
STEP = 4.0
NODES = 8
SLABS = 16
DEVS = NODES * SLABS
CELLS = 256
FIELDS = SWEEPS + 1
HOPS = (0, 1, 2, 1)
FAR_FIRST = sorted(
    ((k // 4 % 4, k % 4, (k + k // 16) % 4, k // 64) for k in (37 * j % DEVS for j in range(DEVS))),
    key=lambda offset: -sum(HOPS[step] for step in offset[:3]),
)
FAR_FIRST.remove((0, 0, 0, 0))


def radau_value(order, point):
    prev_value = 1.0
    prev_slope = 0.0
    this_value = point
    this_slope = 1.0
    for degree in range(1, order):
        next_value = ((2 * degree + 1) * point * this_value - degree * prev_value) / (degree + 1)
        next_slope = (
            (2 * degree + 1) * (this_value + point * this_slope) - degree * prev_slope
        ) / (degree + 1)
        prev_value, prev_slope = (this_value, this_slope)
        this_value, this_slope = (next_value, next_slope)
    return (this_value - prev_value, this_slope - prev_slope)


def radau_tables(node_total):
    points = []
    for node_index in range(node_total):
        estimate = math.cos(2.0 * math.pi * node_index / (2 * node_total - 1))
        if node_index > 0:
            for repeat in range(60):
                poly_value, poly_slope = radau_value(node_total, estimate)
                estimate = estimate - poly_value / poly_slope
        points.append((estimate + 1.0) / 2.0)
    points = sorted(points)
    quadrature = []
    for row_index in range(node_total):
        entries = []
        for column_index in range(node_total):
            coeffs = [1.0]
            for other_index in range(node_total):
                if other_index != column_index:
                    divisor = points[column_index] - points[other_index]
                    shifted = [0.0] + coeffs
                    widened = coeffs + [0.0]
                    coeffs = [
                        (shifted[place] - points[other_index] * widened[place]) / divisor
                        for place in range(len(shifted))
                    ]
            integral = 0.0
            for place in range(len(coeffs)):
                integral = integral + coeffs[place] * points[row_index] ** (place + 1) / (place + 1)
            entries.append(integral)
        quadrature.append(entries)
    return (points, quadrature)


def cas_table(length):
    indices = np.arange(length)
    phases = (indices[:, None] * indices[None, :] % length) * (2.0 * math.pi / length)
    return (np.cos(phases) + np.sin(phases)) / math.sqrt(length)


def eigen_line(length):
    return -4.0 * np.sin(np.arange(length) * (math.pi / length)) ** 2


def pieces(table):
    found = []
    for k in range(3):
        found.append(table.astype(np.float32).astype(BF16))
        table = table - found[-1].astype(np.float64)
    return found


def tables():
    line = cas_table(CELLS)
    parts = pieces(line)
    right = np.concatenate([part[h] for h in (slice(0, 128), slice(128, 256)) for part in parts], 0)
    left = np.concatenate(parts, 1)
    cas_x = cas_table(64)
    cross = np.zeros((2, 64, SLABS, 2, 4))
    for row in range(2):
        cross[row, :, :, row, :] = cas_x.reshape(64, SLABS, 4)
    cross = cross.reshape(128, 128)
    forward = np.concatenate(pieces(cross), 1)
    back = np.concatenate(pieces(cross.T), 1)
    lam_x = np.broadcast_to((STEP * eigen_line(64))[:, None], (64, 128)).astype(np.float32)
    lam_z = np.broadcast_to((STEP * eigen_line(CELLS)).reshape(2, 1, 128), (2, 8, 128)).astype(np.float32)
    lam_y = np.broadcast_to((STEP * eigen_line(CELLS)).reshape(DEVS, 2, 1), (DEVS, 2, 128)).astype(np.float32)
    return right, left, forward, back, lam_x, lam_z, lam_y


def split(value, axis):
    high = value.astype(BF16)
    low = (value - high.astype(F32)).astype(BF16)
    return jnp.concatenate([high, low, high], axis)


def split_fine(value, axis):
    high = value.astype(BF16)
    value = value - high.astype(F32)
    mid = value.astype(BF16)
    low = (value - mid.astype(F32)).astype(BF16)
    return jnp.concatenate([high, high, mid, high, mid, low], axis)


ROUGH = (0, 0, 1)
FINE = (0, 1, 0, 2, 1, 0)


def across(ref, order, width, rows=slice(None)):
    return jnp.concatenate([ref[rows, width * k : width * k + width] for k in order], 1)


def down(ref, order):
    return jnp.concatenate([ref[384 * h + 128 * k : 384 * h + 128 * k + 128, :] for h in range(2) for k in order], 0)


def split_halves(first, second):
    return jnp.concatenate([split(first, 1), split(second, 1)], 1)


def matmul(a, b):
    return jnp.dot(a, b, preferred_element_type=F32)


def kernel(
    points, quadrature,
    sec_hbm, ini_hbm, right_hbm, left_hbm, fwd_hbm, back_hbm, lam_x_hbm, lam_z_hbm, lam_y_hbm,
    first, last, peak,
    sec, ini, right, left, fwd, back, lam_x, lam_z, lam_y,
    rows, rows0, sent, sent0, got, got0, modes, modes0, spect, bsent, bgot, peak_sent, peak_got, peak_all,
    in_sem, send_sem, send0_sem, got_sem, got0_sem, bsend_sem, bgot_sem, psend_sem, pgot_sem,
):
    here = tuple(lax.axis_index(a) for a in AXES)
    my_node = here[0] * 4 + here[1]
    my_slab = (here[2] * 4 + here[3]) * 2 + here[4]
    me = my_node * SLABS + my_slab
    my_y = here[0] * 2 + here[2]

    loads = [
        pltpu.make_async_copy(src, dst, in_sem.at[i])
        for i, (src, dst) in enumerate([
            (left_hbm, left), (sec_hbm.at[0], sec), (right_hbm, right), (ini_hbm, ini), (fwd_hbm, fwd),
            (back_hbm, back), (lam_x_hbm, lam_x), (lam_z_hbm, lam_z), (lam_y_hbm.at[me], lam_y),
        ])
    ]

    def flat(t):
        return (((t[0] * 4 + t[1]) * 2 + t[2]) * 4 + t[3]) * 2 + t[4]

    cores = (here[4], 1 - here[4])
    planes = [lax.rem(my_y + k, 4) for k in range(4)]
    planes = [(y // 2, lax.rem(y, 2)) for y in planes]
    widths = [lax.rem(here[3] + k, 4) for k in range(4)]
    depths = [lax.rem(here[1] + k, 4) for k in range(4)]

    def far_first(visit):
        for y, z, x, core in FAR_FIRST:
            visit((planes[y][0], depths[z], planes[y][1], widths[x], cores[core]))

    barrier = pltpu.get_barrier_semaphore()

    for load in loads:
        load.start()
    far_first(lambda t: pl.semaphore_signal(barrier, inc=1, device_id=t, device_id_type=MESH))

    def put(buf, x, count, value):
        for h in range(2):
            buf[h, pl.ds(x, count, stride=4), :] = value[:, 128 * h : 128 * h + 128]

    loads[0].wait()
    loads[1].wait()
    for x in range(4):
        put(rows.at[0], x, CELLS, matmul(across(left, FINE, CELLS), split_fine(sec[x], 0)))
    loads[2].wait()
    for b in range(4):
        part = [split_fine(rows[0, h, pl.ds(CELLS * b, CELLS), :], 1) for h in range(2)]
        part = matmul(jnp.concatenate(part, 1), down(right, FINE))
        for h in range(2):
            sent[h, pl.ds(32 * b, 32)] = part[:, 128 * h : 128 * h + 128].reshape(32, 8, 128)
    pl.semaphore_wait(barrier, DEVS - 1)

    def spread(src, dst, s_sem, r_sem):
        far_first(
            lambda t: pltpu.make_async_remote_copy(
                src.at[flat(t)], dst.at[me], s_sem, r_sem, device_id=t, device_id_type=MESH
            ).start()
        )
        dst[me] = src[me]

    def all_but_one(buf, count, sem):
        view = buf.at[pl.ds(0, count - 1)]
        pltpu.make_async_copy(view, view, sem).wait()

    spread(sent.at[0], got.at[0], send_sem.at[0], got_sem.at[0])
    loads[3].wait()
    mine = across(left, FINE, CELLS, pl.ds(pl.multiple_of(my_node * 32, 32), 32))
    for x in range(4):
        put(rows0, x, 32, matmul(mine, split_fine(ini[x], 0)))
    part = jnp.concatenate([split_fine(rows0[h], 1) for h in range(2)], 1)
    part = matmul(part, down(right, FINE))
    for h in range(2):
        sent0[h] = part[:, 128 * h : 128 * h + 128].reshape(16, 8, 128)

    for h in range(2):
        for k in range(1, SLABS):
            x = lax.rem(here[3] + k, 4)
            t = (here[0], here[1], here[2] if k < 8 else 1 - here[2], x, cores[k // 4 % 2])
            pltpu.make_async_remote_copy(
                sent0.at[h, (t[2] * 4 + t[3]) * 2 + t[4]], got0.at[h, my_slab], send0_sem.at[h], got0_sem.at[h],
                device_id=t, device_id_type=MESH,
            ).start()
        got0[h, my_slab] = sent0[h, my_slab]
    spread(sent.at[1], got.at[1], send_sem.at[1], got_sem.at[1])

    for load in loads[4:]:
        load.wait()

    def enter(h):
        all_but_one(got0.at[h], SLABS, got0_sem.at[h])
        all_but_one(got.at[h], DEVS, got_sem.at[h])
        modes0[...] = matmul(across(fwd, FINE, 128), split_fine(got0[h].reshape(128, 128), 0))
        for n in range(0, NODES, 2):
            pair = [got[h, pl.ds(SLABS * (n + k), SLABS)].reshape(128, 128) for k in range(2)]
            modes[:, 128 * n : 128 * n + 256] = matmul(across(fwd, FINE, 128), split_fine(jnp.concatenate(pair, 1), 0))

    def sweep(k, h):
        lam_0 = [lam_z[h] + lam_y[row : row + 1, :] for row in range(2)]

        def one(i, carry):
            lam_1 = lam_x[pl.ds(pl.multiple_of(8 * i, 8), 8), :]
            for row in range(2):
                r = pl.multiple_of(64 * row + 8 * i, 8)
                lam = lam_1 + lam_0[row]
                start = modes0[pl.ds(r, 8), :]
                value = [modes[pl.ds(r, 8), 128 * m : 128 * m + 128] for m in range(NODES)]
                slope = [lam * v for v in value]
                for m in range(NODES):
                    total = start - value[m]
                    for j in range(NODES):
                        total = total + quadrature[m][j] * slope[j]
                    spect[pl.ds(r, 8), 128 * m : 128 * m + 128] = total
                    modes[pl.ds(r, 8), 128 * m : 128 * m + 128] = value[m] + total / (
                        1.0 - (points[m] / (k + 1.0)) * lam
                    )
            return carry

        lax.fori_loop(0, 8, one, 0)

    def make(f, h):
        source = spect if f < SWEEPS else modes
        for n in range(0, NODES, 2):
            pair = matmul(across(back, ROUGH, 128), split(source[:, 128 * n : 128 * n + 256], 0))
            for k in range(2):
                block = pair[:, 128 * k : 128 * k + 128]
                if f < 2:
                    bsent[f, h, pl.ds(SLABS * (n + k), SLABS)] = block.reshape(SLABS, 8, 128)
                else:
                    rows[f - 2, h, pl.ds(128 * (n + k), 128), :] = block

    def make_z(f):
        for b in range(4):
            part = split_halves(*(rows[f - 2, h, pl.ds(CELLS * b, CELLS), :] for h in range(2)))
            part = matmul(part, down(right, ROUGH))
            for h in range(2):
                bsent[f, h, pl.ds(32 * b, 32)] = part[:, 128 * h : 128 * h + 128].reshape(32, 8, 128)

    def give(f, h):
        spread(bsent.at[f, h], bgot.at[f, h], bsend_sem.at[f, h], bgot_sem.at[f, h])

    enter(0)
    for f in range(FIELDS):
        if f < SWEEPS:
            sweep(f, 0)
        make(f, 0)
        if f < 2:
            give(f, 0)
    enter(1)
    for f in range(FIELDS):
        if f < SWEEPS:
            sweep(f, 1)
        make(f, 1)
        if f >= 2:
            make_z(f)
            give(f, 0)
        if f < SWEEPS:
            give(f, 1)

    def ready(f, h):
        all_but_one(bgot.at[f, h], DEVS, bgot_sem.at[f, h])

    def plane(f, h, x):
        return bgot.at[f, h].reshape(4 * CELLS, 128)[pl.ds(x, CELLS, stride=4), :]

    def pairs(f, h):
        for x in range(0, 4, 2):
            part = jnp.concatenate([plane(f, h, x + k) for k in range(2)], 1)
            part = matmul(across(left, ROUGH, CELLS), split(part, 0))
            yield x, part[:, :128]
            yield x + 1, part[:, 128:]

    def peak_of(parts):
        parts = [jnp.max(jnp.abs(part).reshape(32, 8, part.shape[1]), axis=0) for part in parts]
        return jnp.max(functools.reduce(jnp.maximum, parts))

    lane = lax.broadcasted_iota(jnp.int32, (1, 128), 1)
    peaks = jnp.zeros((1, 128), F32)
    for f in range(2):
        ready(f, 0)
        ready(f, 1)
        parts = []
        for x in range(4):
            part = jnp.concatenate([plane(f, h, x) for h in range(2)], 1)
            part = matmul(across(left, ROUGH, CELLS), split(part, 0))
            parts.append(matmul(split_halves(part[:, :128], part[:, 128:]), down(right, ROUGH)))
        peaks = jnp.where(lane == f, peak_of(parts), peaks)
    for h in range(2):
        ready(2, h)
        top = peak_of([part for x, part in pairs(2, h)])
        peaks = jnp.maximum(peaks, jnp.where(lane == 2, top, 0.0))
    peak_sent[0] = peaks

    place = here[1] * 4 + here[3]
    for k in range(1, 16):
        pltpu.make_async_remote_copy(
            peak_sent.at[0], peak_got.at[place], psend_sem.at[0], pgot_sem.at[0],
            device_id=(here[0], depths[k // 4], here[2], widths[k % 4], here[4]), device_id_type=MESH,
        ).start()
    peak_got[place] = peaks
    give(SWEEPS, 1)
    all_but_one(peak_got, 16, pgot_sem.at[0])
    peaks = jnp.max(peak_got[...], axis=0)
    peak_sent[1] = peaks
    place = my_y * 2 + here[4]
    for k in range(1, 8):
        pltpu.make_async_remote_copy(
            peak_sent.at[1], peak_all.at[place], psend_sem.at[1], pgot_sem.at[1],
            device_id=(planes[k // 2][0], here[1], planes[k // 2][1], here[3], cores[k % 2]),
            device_id_type=MESH,
        ).start()
    peak_all[place] = peaks
    ready(SWEEPS, 0)
    for x, part in pairs(SWEEPS, 0):
        first[x] = part
    all_but_one(peak_all, 8, pgot_sem.at[1])
    peak[...] = jnp.max(peak_all[...], axis=0)
    for h in range(2):
        all_but_one(sent0.at[h], SLABS, send0_sem.at[h])
        all_but_one(sent.at[h], DEVS, send_sem.at[h])
        for f in range(FIELDS):
            all_but_one(bsent.at[f, h], DEVS, bsend_sem.at[f, h])
    all_but_one(peak_got, 16, psend_sem.at[0])
    all_but_one(peak_all, 8, psend_sem.at[1])
    ready(SWEEPS, 1)
    for x, part in pairs(SWEEPS, 1):
        last[x] = part


def finish(first, last, peak, out_hbm, res_hbm, res, out_sem):
    copies = [
        pltpu.make_async_copy(part, out_hbm.at[0, :, :, pl.ds(128 * h, 128)], out_sem.at[h])
        for h, part in enumerate((first, last))
    ]
    for copy in copies:
        copy.start()
    lane = lax.broadcasted_iota(jnp.int32, (1, 128), 1)
    for f in range(SWEEPS):
        res[f] = jnp.max(jnp.where(lane == f, peak[...], 0.0))
    copies.append(pltpu.make_async_copy(res, res_hbm, out_sem.at[2]))
    copies[2].start()
    for copy in copies:
        copy.wait()


def on_device(initial, sections):
    points, quadrature = radau_tables(NODES)
    any_space = pl.BlockSpec(memory_space=pl.ANY)
    dma = pltpu.SemaphoreType.DMA
    parts = [jnp.asarray(t) for t in tables()]
    vmem = pltpu.VMEM
    whole = pl.BlockSpec(memory_space=pltpu.VMEM)
    pinned = pl.BlockSpec(memory_space=pltpu.HBM)
    found = pl.pallas_call(
        functools.partial(kernel, points, quadrature),
        out_shape=(
            jax.ShapeDtypeStruct((4, CELLS, 128), F32),
            jax.ShapeDtypeStruct((4, CELLS, 128), F32),
            jax.ShapeDtypeStruct((1, 128), F32),
        ),
        in_specs=[pinned] * 9,
        out_specs=(whole,) * 3,
        scratch_shapes=[
            vmem((4, CELLS, CELLS), F32),
            vmem((4, CELLS, CELLS), F32),
            vmem((3 * CELLS, CELLS), BF16),
            vmem((CELLS, 3 * CELLS), BF16),
            vmem((128, 384), BF16),
            vmem((128, 384), BF16),
            vmem((64, 128), F32),
            vmem((2, 8, 128), F32),
            vmem((2, 128), F32),
            vmem((2, 2, 4 * CELLS, 128), F32),
            vmem((2, 128, 128), F32),
            vmem((2, DEVS, 8, 128), F32),
            vmem((2, SLABS, 8, 128), F32),
            vmem((2, DEVS, 8, 128), F32),
            vmem((2, SLABS, 8, 128), F32),
            vmem((128, NODES * 128), F32),
            vmem((128, 128), F32),
            vmem((128, NODES * 128), F32),
            vmem((FIELDS, 2, DEVS, 8, 128), F32),
            vmem((FIELDS, 2, DEVS, 8, 128), F32),
            vmem((2, 1, 128), F32),
            vmem((16, 1, 128), F32),
            vmem((8, 1, 128), F32),
            dma((9,)),
            dma((2,)),
            dma((2,)),
            dma((2,)),
            dma((2,)),
            dma((FIELDS, 2)),
            dma((FIELDS, 2)),
            dma((2,)),
            dma((2,)),
        ],
        compiler_params=pltpu.CompilerParams(
            collective_id=0, has_side_effects=True, vmem_limit_bytes=30 << 20
        ),
        name="sdc",
    )(*(pltpu.with_memory_space_constraint(value, pltpu.HBM) for value in (sections, initial, *parts)))
    return pl.pallas_call(
        finish,
        out_shape=(
            jax.ShapeDtypeStruct(sections.shape, F32),
            jax.ShapeDtypeStruct((SWEEPS,), F32),
        ),
        in_specs=[whole] * 3,
        out_specs=(any_space, any_space),
        scratch_shapes=[pltpu.SMEM((SWEEPS,), F32), dma((3,))],
        compiler_params=pltpu.CompilerParams(vmem_limit_bytes=16 << 20),
        name="finish",
    )(*found)


def solution(mesh):
    torus = Mesh(mesh.devices.reshape(2, 4, 2, 4, 2), AXES)
    return jax.shard_map(
        on_device,
        mesh=torus,
        in_specs=(P(SLAB, None, None), P(NODE, SLAB, None, None)),
        out_specs=(P(NODE, SLAB, None, None), P()),
        check_vma=False,
    )
```
